32 devices in a mesh: tmpl: 2 (over core), row: 4 (over z), col: 4 (over y, x).
Axes of the slice: x: 2, y: 2, z: 4, core: 2. Of those that a mesh axis runs over, the one named last changes fastest.
Arguments:
- template_pair: bfloat16 [2, 512, 64, 512], P('tmpl', 'row', None, 'col'), may hold values from -6 to 6
- trunk: bfloat16 [512, 128, 512], P('row', None, 'col'), may hold values from -6 to 6
- coverage: int32 [2, 512], replicated, may hold values from 0 to 1, as said below
- chain_ids: int32 [512], replicated, may hold values from 0 to 3, never falling along the last dimension, each value on 1 to 256 neighbouring positions
- chain_vec: float32 [64], replicated, may hold values from -4 to 4
- trunk_weights: bfloat16 [64, 128], replicated, may hold values from -0.5 to 0.5
- proj_weights: bfloat16 [2, 5, 64, 64], replicated, may hold values from -0.75 to 0.75
- out_weights: bfloat16 [2, 64, 64], replicated, may hold values from -0.75 to 0.75
- final_weights: bfloat16 [128, 64], replicated, may hold values from -0.75 to 0.75
Outputs:
- trunk_out: bfloat16 [512, 128, 512], P('row', None, 'col')
The draws below stay inside these ranges and needn't reach their ends.
Inputs may be any that keep to these rules, and one draw needn't show every extreme that they name: coverage[t, i] is 1 where template t covers token i, else 0; how densely a template covers tokens is drawn anew for each block of 128 consecutive tokens. `chain_ids`: chain ids never fall along the tokens.
All inputs are finite; a program needn't handle non-finite values.
Results may differ from the reference program's by a relative error of at most 0.008.
Values may be sent and summed in bfloat16 or wider, within the bound.
No kernel may reach another device: no remote copies, remote signals or barrier semaphores. Data moves between devices by JAX's collectives and lax.ppermute only.
A program may use at most 128 MiB of HBM per device.

```python
import math
import jax
import jax.numpy as jnp
import numpy as np
from jax import lax

C = 64
CZ = 128
N = 512
TEMPLATES = 2
ROWS = 128
COLS = 128
N_ROW = 4
N_COL = 4


def draw_coverage(key, part):
    level_key = jax.random.fold_in(key, 11)
    coin_key = jax.random.fold_in(key, 23)
    levels = jax.random.randint(level_key, (TEMPLATES, N // ROWS), 0, 4)
    spread_levels = jnp.repeat(levels, ROWS, axis=1)
    coins = jax.random.randint(coin_key, (TEMPLATES, N), 0, 4)
    return (coins < spread_levels).astype(jnp.int32)


def level_of(key, extent, cuts, smallest, high):
    factor_of, own = 1.0, jax.random.fold_in(key, 6)
    for position, parts in cuts:
        draws = jnp.exp(jax.random.uniform(jax.random.fold_in(own, position), (parts,), jnp.float32, smallest / len(cuts), high / len(cuts)))
        factor_of = factor_of * jnp.repeat(draws, extent[position] // parts).reshape([-1 if axis == position else 1 for axis in range(len(extent))])
    return factor_of


def profile(number_of, total, most, skew):
    loads = [(1 << 20) // math.isqrt(grade ** skew) + 1 for grade in range(2, number_of + 1)]
    rest, holding = total - most - (number_of - 1), [1] * (number_of - 1)
    while rest > 0:
        candidates = [i for i in range(number_of - 1) if holding[i] < most]
        mass, budget = sum([loads[i] for i in candidates]), rest
        for i in candidates:
            more = min(most - holding[i], max(1, budget * loads[i] // mass), rest)
            holding[i] = holding[i] + more
            rest = rest - more
    return np.array([most] + holding)


def ragged(key, amount, total, most, skew):
    if amount == 2:
        one = jax.random.randint(key, (), max(1, total - most), min(most, total - 1) + 1)
        return jnp.stack([one, total - one])
    sizes = jnp.asarray(profile(amount, total, most, skew), jnp.int32)
    couples = (amount - 1) // 2
    source_of, sink = sizes[1:1 + 2 * couples:2], sizes[2:2 + 2 * couples:2]
    room = jnp.minimum(source_of - 1, most - sink)
    shifted = jax.random.randint(jax.random.fold_in(key, 1), (couples,), 0, 1 << 20) % (room + 1)
    sizes = sizes.at[1:1 + 2 * couples:2].set(source_of - shifted).at[2:2 + 2 * couples:2].set(sink + shifted)
    return sizes[jax.random.permutation(jax.random.fold_in(key, 2), amount)]


def gaussian(stream_key, extent, deviation, most, split=(), dtype=jnp.bfloat16):
    result = deviation * jax.random.normal(stream_key, extent, jnp.float32)
    if split:
        result = result * level_of(stream_key, extent, split, -0.22, 0.18)
    return jnp.clip(result, -most, most).astype(dtype)


def setup_inputs(seed: int = 0) -> dict:
    splits = jax.random.split(jax.random.key(seed), 10)
    template_pair = gaussian(splits[0], (TEMPLATES, N, C, N), 1.0, 6.0, ((0, 2), (1, 4), (3, 4)))
    trunk = gaussian(splits[1], (N, CZ, N), 1.0, 6.0, ((0, 4), (2, 4)))
    coverage = draw_coverage(jax.random.fold_in(splits[9], 71), 0)
    chain_ids = jnp.searchsorted(jnp.cumsum(ragged(splits[3], 4, N, N // 2, 2)), jnp.arange(N), side="right").astype(jnp.int32)
    chain_vec = gaussian(splits[4], (C,), 1.0, 4.0, (), jnp.float32)
    trunk_weights = gaussian(splits[5], (C, CZ), CZ ** -0.5, 0.5)
    proj_weights = gaussian(splits[6], (2, 5, C, C), C ** -0.5, 0.75)
    out_weights = gaussian(splits[7], (2, C, C), C ** -0.5, 0.75)
    final_weights = gaussian(splits[8], (CZ, C), C ** -0.5, 0.75)
    return {"template_pair": template_pair, "trunk": trunk, "coverage": coverage, "chain_ids": chain_ids, "chain_vec": chain_vec, "trunk_weights": trunk_weights, "proj_weights": proj_weights, "out_weights": out_weights, "final_weights": final_weights}


epsilon = 1e-05

def channel_norm(values):
    centre = lax.optimization_barrier(jnp.mean(values, axis=1, keepdims=True))
    centred = values - centre
    spread = lax.optimization_barrier(jnp.mean(centred * centred, axis=1, keepdims=True))
    return centred * lax.rsqrt(spread + epsilon)

def project(weights, values):
    return jnp.einsum('dc,icj->idj', weights.astype(jnp.float32), values.astype(jnp.float32))

def rounded(values):
    return lax.optimization_barrier(values.astype(jnp.bfloat16)).astype(jnp.float32)

def gated_pair(pair_rep, pair_mask, weights):
    normed = channel_norm(pair_rep.astype(jnp.float32)).astype(jnp.bfloat16)
    pieces = [project(weights[number], normed) for number in range(5)]
    weighted = pair_mask[:, None, :]
    left_proj = (weighted * jax.nn.sigmoid(pieces[0]) * pieces[1]).astype(jnp.bfloat16)
    right_proj = (weighted * jax.nn.sigmoid(pieces[2]) * pieces[3]).astype(jnp.bfloat16)
    return (left_proj, right_proj, pieces[4])

def apply_update(pair_rep, tri_sum, gate_proj, weights):
    tri_norm = channel_norm(tri_sum).astype(jnp.bfloat16)
    update = jax.nn.sigmoid(gate_proj) * project(weights, tri_norm)
    return (pair_rep.astype(jnp.float32) + update).astype(jnp.bfloat16)

def outgoing_sum(left_proj, right_proj):
    tri_sum = jnp.zeros((N, left_proj.shape[1], N), jnp.float32)
    for block_number in range(N_COL):
        lower = block_number * COLS
        left_block = left_proj[:, :, lower:lower + COLS].astype(jnp.float32)
        right_block = right_proj[:, :, lower:lower + COLS].astype(jnp.float32)
        tri_sum = tri_sum + rounded(jnp.einsum('ick,jck->icj', left_block, right_block))
    return tri_sum

def incoming_sum(left_proj, right_proj):
    tri_sum = jnp.zeros((N, left_proj.shape[1], N), jnp.float32)
    for block_number in range(N_ROW):
        lower = block_number * ROWS
        left_block = left_proj[lower:lower + ROWS].astype(jnp.float32)
        right_block = right_proj[lower:lower + ROWS].astype(jnp.float32)
        tri_sum = tri_sum + rounded(jnp.einsum('kci,kcj->icj', left_block, right_block))
    return tri_sum

def reference(template_pair, trunk, coverage, chain_ids, chain_vec, trunk_weights, proj_weights, out_weights, final_weights):
    same_chain = (chain_ids[:, None] == chain_ids[None, :]).astype(jnp.float32)
    cover_float = coverage.astype(jnp.float32)
    cover_count = lax.optimization_barrier(jnp.sum(cover_float[:, :, None] * cover_float[:, None, :], axis=0))
    trunk_proj = project(trunk_weights, channel_norm(trunk.astype(jnp.float32)))
    pooled = jnp.zeros((N, template_pair.shape[2], N), jnp.float32)
    for template_index in range(TEMPLATES):
        pair_mask = cover_float[template_index][:, None] * cover_float[template_index][None, :]
        pair_rep = (template_pair[template_index].astype(jnp.float32) + same_chain[:, None, :] * chain_vec[None, :, None] + trunk_proj).astype(jnp.bfloat16)
        left_proj, right_proj, gate_proj = gated_pair(pair_rep, pair_mask, proj_weights[0])
        pair_rep = apply_update(pair_rep, outgoing_sum(left_proj, right_proj), gate_proj, out_weights[0])
        left_proj, right_proj, gate_proj = gated_pair(pair_rep, pair_mask, proj_weights[1])
        pair_rep = apply_update(pair_rep, incoming_sum(left_proj, right_proj), gate_proj, out_weights[1])
        pooled = pooled + pair_mask[:, None, :] * channel_norm(pair_rep.astype(jnp.float32))
    hidden = jax.nn.relu(pooled / jnp.maximum(cover_count, 1.0)[:, None, :]).astype(jnp.bfloat16)
    return (trunk.astype(jnp.float32) + project(final_weights, hidden)).astype(jnp.bfloat16)
```

```python
import functools

import jax
import jax.numpy as jnp
from jax import lax
from jax.experimental import pallas as pl
from jax.experimental.pallas import tpu as pltpu
from jax.sharding import PartitionSpec as P

epsilon = 1e-05
GROUP = 16
F32 = jnp.float32
BF16 = jnp.bfloat16


def sigmoid(x):
    return 0.5 * jnp.tanh(0.5 * x) + 0.5


def norm_rows(x):
    scale = 1.0 / x.shape[0]
    centred = x - jnp.sum(x, axis=0, keepdims=True) * scale
    spread = jnp.sum(centred * centred, axis=0, keepdims=True) * scale
    return centred * lax.rsqrt(spread + epsilon)


def project_rows(weights, rows):
    wide = jnp.concatenate(rows, axis=1)
    out = jnp.dot(weights, wide, preferred_element_type=F32)
    cols = rows[0].shape[1]
    return [out[:, n * cols : (n + 1) * cols] for n in range(len(rows))]


def emit_gated(reps, masks, first, weights_ref, gate_ref, scratch):
    channels = reps[0].shape[0]
    normed = [norm_rows(rep).astype(BF16) for rep in reps]
    for half in range(0, len(reps), 2):
        pieces = project_rows(weights_ref[...], normed[half : half + 2])
        for n, piece in enumerate(pieces):
            p = [piece[k * channels : (k + 1) * channels] for k in range(5)]
            at = first + half + n
            rows = pl.ds(pl.multiple_of(at * channels, channels), channels)
            mask = masks[half + n]
            scratch[0, rows, :] = mask * sigmoid(p[0]) * p[1]
            scratch[1, rows, :] = mask * sigmoid(p[2]) * p[3]
            gate_ref[at] = sigmoid(p[4]).astype(gate_ref.dtype)


def store_by_channel(scratch, pair_ref):
    slots, _, per_slot = pair_ref.shape[:3]
    channels = slots * per_slot
    for side in range(2):
        for channel in range(channels):
            rows = scratch[side, pl.ds(channel, GROUP, stride=channels), :]
            pair_ref[channel // per_slot, side, channel % per_slot] = rows.astype(BF16)


STEP = 4


def pre_kernel(cover_ref, chain_ref, tp_ref, trunk_ref, cover_cols_ref, chain_cols_ref, chain_vec_ref,
               trunk_weights_ref, weights_ref, pair_ref, rep_ref, gate_ref, scratch):
    base = pl.program_id(0) * GROUP
    cols = tp_ref.shape[3]
    channels = tp_ref.shape[2]
    trunk_weights = trunk_weights_ref[...]
    weight_sums = jnp.sum(trunk_weights.astype(F32), axis=1, keepdims=True)

    def body(step, carry):
        first = step * STEP
        reps, masks = [], []
        rows = [trunk_ref[first + n] for n in range(STEP)]
        projected = []
        for half in range(0, STEP, 2):
            projected += project_rows(trunk_weights, rows[half : half + 2])
        for n in range(STEP):
            at = first + n
            values = rows[n].astype(F32)
            scale = 1.0 / values.shape[0]
            centre = jnp.sum(values, axis=0, keepdims=True) * scale
            centred = values - centre
            spread = jnp.sum(centred * centred, axis=0, keepdims=True) * scale
            trunk_proj = (projected[n] - weight_sums * centre) * lax.rsqrt(spread + epsilon)
            same = (chain_cols_ref[...] == chain_ref[base + at]).astype(F32)
            rep = (tp_ref[0, at].astype(F32) + same * chain_vec_ref[...] + trunk_proj).astype(BF16)
            rep_ref[at] = rep
            reps.append(rep.astype(F32))
            masks.append(cover_cols_ref[...] * cover_ref[base + at])
        emit_gated(reps, masks, first, weights_ref, gate_ref, scratch)
        return carry

    lax.fori_loop(0, GROUP // STEP, body, 0)
    store_by_channel(scratch, pair_ref)


def load_tri(tri_ref, tri_scratch):
    channels = tri_ref.shape[0]
    scale = 1.0 / channels
    half = GROUP // 2
    for part in range(2):
        rows = slice(part * half, (part + 1) * half)
        total = jnp.zeros((half, tri_ref.shape[2]), F32)
        for channel in range(channels):
            total += tri_ref[channel].astype(F32)[rows]
        centre = total * scale
        total = jnp.zeros_like(total)
        for channel in range(channels):
            centred = tri_ref[channel].astype(F32)[rows] - centre
            total += centred * centred
        inverse = lax.rsqrt(total * scale + epsilon)
        for channel in range(channels):
            tri_scratch[channel * GROUP + part * half : channel * GROUP + (part + 1) * half, :] = (
                tri_ref[channel].astype(F32)[rows] - centre
            ) * inverse


def updated_rows(first, tri_scratch, rep_ref, gate_ref, out_weights_ref):
    channels = rep_ref.shape[1]
    normed = [
        tri_scratch[pl.ds(first + n, channels, stride=GROUP), :].astype(BF16) for n in range(STEP)
    ]
    projected = []
    for half in range(0, STEP, 2):
        projected += project_rows(out_weights_ref[...], normed[half : half + 2])
    return [
        (rep_ref[first + n].astype(F32) + gate_ref[first + n].astype(F32) * projected[n]).astype(BF16)
        for n in range(STEP)
    ]


def mid_kernel(cover_ref, tri_ref, rep_in_ref, gate_in_ref, cover_cols_ref, out_weights_ref, weights_ref,
               pair_ref, rep_ref, gate_ref, scratch, tri_scratch):
    base = pl.program_id(0) * GROUP
    load_tri(tri_ref, tri_scratch)

    def body(step, carry):
        first = step * STEP
        rows = updated_rows(first, tri_scratch, rep_in_ref, gate_in_ref, out_weights_ref)
        masks = []
        for n in range(STEP):
            rep_ref[first + n] = rows[n]
            masks.append(cover_cols_ref[...] * cover_ref[base + first + n])
        emit_gated([row.astype(F32) for row in rows], masks, first, weights_ref, gate_ref, scratch)
        return carry

    lax.fori_loop(0, GROUP // STEP, body, 0)
    store_by_channel(scratch, pair_ref)


def last_kernel(cover_ref, tri_ref, rep_in_ref, gate_in_ref, cover_cols_ref, out_weights_ref, pooled_ref, tri_scratch):
    base = pl.program_id(0) * GROUP
    load_tri(tri_ref, tri_scratch)

    def body(step, carry):
        first = step * STEP
        rows = updated_rows(first, tri_scratch, rep_in_ref, gate_in_ref, out_weights_ref)
        for n in range(STEP):
            mask = cover_cols_ref[...] * cover_ref[base + first + n]
            pooled_ref[first + n] = (mask * norm_rows(rows[n].astype(F32))).astype(BF16)
        return carry

    lax.fori_loop(0, GROUP // STEP, body, 0)


def finish_kernel(cover_ref, mine_ref, other_ref, trunk_ref, cover_cols_ref, final_weights_ref, out_ref):
    base = pl.program_id(0) * GROUP

    def body(step, carry):
        first = step * STEP
        hidden = []
        for n in range(STEP):
            at = first + n
            count = sum(
                cover_cols_ref[t : t + 1, :] * cover_ref[t, base + at] for t in range(cover_cols_ref.shape[0])
            )
            pooled = mine_ref[at].astype(F32) + other_ref[at].astype(F32)
            hidden.append(jnp.maximum(pooled / jnp.maximum(count, 1.0), 0.0).astype(BF16))
        for half in range(0, STEP, 2):
            for n, row in enumerate(project_rows(final_weights_ref[...], hidden[half : half + 2])):
                at = first + half + n
                out_ref[at] = (trunk_ref[at].astype(F32) + row).astype(BF16)
        return carry

    lax.fori_loop(0, GROUP // STEP, body, 0)


def outgoing_kernel(rows_n, cols_n, pair_ref, tri_ref):
    height = pair_ref.shape[3]
    left = jnp.concatenate(
        [
            jnp.concatenate([pair_ref[r * cols_n + c, 0, 0] for c in range(cols_n)], axis=1)
            for r in range(rows_n)
        ],
        axis=0,
    )
    right = jnp.concatenate(
        [
            jnp.concatenate([pair_ref[r * cols_n + c, 1, 0] for c in range(cols_n)], axis=1)
            for r in range(rows_n)
        ],
        axis=0,
    )
    out = lax.dot_general(left, right, (((1,), (1,)), ((), ())), preferred_element_type=F32)
    width = tri_ref.shape[3]
    for r in range(rows_n):
        for c in range(cols_n):
            tri_ref[r * cols_n + c, 0] = out[
                r * height : (r + 1) * height, c * width : (c + 1) * width
            ].astype(BF16)


def incoming_kernel(rows_n, cols_n, pair_ref, tri_ref):
    left = jnp.concatenate(
        [
            jnp.concatenate([pair_ref[r * cols_n + c, 0, 0] for c in range(cols_n)], axis=1)
            for r in range(rows_n)
        ],
        axis=0,
    )
    right = jnp.concatenate(
        [
            jnp.concatenate([pair_ref[r * cols_n + c, 1, 0] for c in range(cols_n)], axis=1)
            for r in range(rows_n)
        ],
        axis=0,
    )
    out = lax.dot_general(left, right, (((0,), (0,)), ((), ())), preferred_element_type=F32)
    height, width = tri_ref.shape[2:]
    for r in range(rows_n):
        for c in range(cols_n):
            tri_ref[r * cols_n + c, 0] = out[
                r * height : (r + 1) * height, c * width : (c + 1) * width
            ].astype(BF16)


def triangle(body, rows_n, cols_n, pairs, name):
    slots, _, per_slot, height, width = pairs.shape
    return pl.pallas_call(
        functools.partial(body, rows_n, cols_n),
        grid=(per_slot,),
        in_specs=[pl.BlockSpec((slots, 2, 1, height, width), lambda c: (0, 0, c, 0, 0))],
        out_specs=pl.BlockSpec((slots, 1, height, width), lambda c: (0, c, 0, 0)),
        out_shape=jax.ShapeDtypeStruct((slots, per_slot, height, width), BF16),
        name=name,
    )(pairs)


SMEM = pl.BlockSpec(memory_space=pltpu.SMEM)


def whole_block(array):
    zeros = (0,) * array.ndim
    return pl.BlockSpec(array.shape, lambda g: zeros)


def rows_block(*rest):
    zeros = (0,) * len(rest)
    return pl.BlockSpec((GROUP,) + rest, lambda g: (g,) + zeros)


def per_device(
    template_pair,
    trunk,
    coverage,
    chain_ids,
    chain_vec,
    trunk_weights,
    proj_weights,
    out_weights,
    final_weights,
):
    tile_rows, trunk_channels, tile_cols = trunk.shape
    channels = template_pair.shape[2]
    rows_n, cols_n = lax.axis_size("row"), lax.axis_size("col")
    slots = rows_n * cols_n
    per_slot = channels // slots
    grid = (tile_rows // GROUP,)
    row_start = lax.axis_index("row") * tile_rows
    col_start = lax.axis_index("col") * tile_cols
    cover_float = coverage.astype(F32)
    cover_rows = lax.dynamic_slice_in_dim(cover_float, row_start, tile_rows, 1)
    cover_cols = lax.dynamic_slice_in_dim(cover_float, col_start, tile_cols, 1)
    chain_rows = lax.dynamic_slice_in_dim(chain_ids, row_start, tile_rows, 0)
    chain_cols = lax.dynamic_slice_in_dim(chain_ids, col_start, tile_cols, 0)[None]
    template_index = lax.axis_index("tmpl")
    my_rows = lax.dynamic_index_in_dim(cover_rows, template_index, 0, keepdims=False)
    my_cols = lax.dynamic_index_in_dim(cover_cols, template_index, 0, keepdims=True)
    stacked = proj_weights.reshape(2, 5 * channels, channels)

    pair_spec = pl.BlockSpec((slots, 2, per_slot, GROUP, tile_cols), lambda g: (0, 0, 0, g, 0))
    pair_shape = jax.ShapeDtypeStruct((slots, 2, per_slot, tile_rows, tile_cols), BF16)
    rep_spec = rows_block(channels, tile_cols)
    rep_shape = jax.ShapeDtypeStruct((tile_rows, channels, tile_cols), BF16)
    trunk_spec = rows_block(trunk_channels, tile_cols)
    tri_spec = pl.BlockSpec((channels, GROUP, tile_cols), lambda g: (0, g, 0))
    scratch = pltpu.VMEM((2, GROUP * channels, tile_cols), F32)
    tri_scratch = pltpu.VMEM((channels * GROUP, tile_cols), F32)
    gated_outs = dict(
        out_specs=[pair_spec, rep_spec, rep_spec], out_shape=[pair_shape, rep_shape, rep_shape]
    )

    def exchange(values):
        return lax.all_to_all(values, ("row", "col"), 0, 0, tiled=True)

    chain_column = chain_vec[:, None]
    pairs, rep, gate = pl.pallas_call(
        pre_kernel,
        grid=grid,
        in_specs=[
            SMEM,
            SMEM,
            pl.BlockSpec((1, GROUP, channels, tile_cols), lambda g: (0, g, 0, 0)),
            trunk_spec,
            whole_block(my_cols),
            whole_block(chain_cols),
            whole_block(chain_column),
            whole_block(trunk_weights),
            whole_block(stacked[0]),
        ],
        scratch_shapes=[scratch],
        name="pre",
        **gated_outs,
    )(my_rows, chain_rows, template_pair, trunk, my_cols, chain_cols, chain_column, trunk_weights, stacked[0])

    tri = exchange(triangle(outgoing_kernel, rows_n, cols_n, exchange(pairs), "outgoing"))
    pairs, rep, gate = pl.pallas_call(
        mid_kernel,
        grid=grid,
        in_specs=[
            SMEM,
            tri_spec,
            rep_spec,
            rep_spec,
            whole_block(my_cols),
            whole_block(out_weights[0]),
            whole_block(stacked[1]),
        ],
        scratch_shapes=[scratch, tri_scratch],
        name="mid",
        **gated_outs,
    )(
        my_rows,
        tri.reshape(channels, tile_rows, tile_cols),
        rep,
        gate,
        my_cols,
        out_weights[0],
        stacked[1],
    )

    tri = exchange(triangle(incoming_kernel, rows_n, cols_n, exchange(pairs), "incoming"))
    pooled = pl.pallas_call(
        last_kernel,
        grid=grid,
        in_specs=[SMEM, tri_spec, rep_spec, rep_spec, whole_block(my_cols), whole_block(out_weights[1])],
        out_specs=rep_spec,
        out_shape=rep_shape,
        scratch_shapes=[tri_scratch],
        name="last",
    )(my_rows, tri.reshape(channels, tile_rows, tile_cols), rep, gate, my_cols, out_weights[1])

    other = lax.ppermute(pooled, "tmpl", [(0, 1), (1, 0)])
    return pl.pallas_call(
        finish_kernel,
        grid=grid,
        in_specs=[SMEM, rep_spec, rep_spec, trunk_spec, whole_block(cover_cols), whole_block(final_weights)],
        out_specs=trunk_spec,
        out_shape=jax.ShapeDtypeStruct(trunk.shape, BF16),
        name="finish",
    )(cover_rows, pooled, other, trunk, cover_cols, final_weights)


def solution(mesh):
    in_specs = (
        P("tmpl", "row", None, "col"),
        P("row", None, "col"),
        P(),
        P(),
        P(),
        P(),
        P(),
        P(),
        P(),
    )
    out_specs = P("row", None, "col")
    return jax.shard_map(
        per_device, mesh=mesh, in_specs=in_specs, out_specs=out_specs, check_vma=False
    )
```

```python
import functools

import jax
import jax.numpy as jnp
from jax import lax
from jax.experimental import pallas as pl
from jax.experimental.pallas import tpu as pltpu
from jax.sharding import PartitionSpec as P

epsilon = 1e-05
GROUP = 16
F32 = jnp.float32
BF16 = jnp.bfloat16


def sigmoid(x):
    return 0.5 * jnp.tanh(0.5 * x) + 0.5


def norm_rows(x):
    scale = 1.0 / x.shape[0]
    centred = x - jnp.sum(x, axis=0, keepdims=True) * scale
    spread = jnp.sum(centred * centred, axis=0, keepdims=True) * scale
    return centred * lax.rsqrt(spread + epsilon)


def project_rows(weights, rows):
    wide = jnp.concatenate(rows, axis=1)
    out = jnp.dot(weights, wide, preferred_element_type=F32)
    cols = rows[0].shape[1]
    return [out[:, n * cols : (n + 1) * cols] for n in range(len(rows))]


def emit_gated(reps, masks, first, weights_ref, gate_ref, scratch):
    channels = reps[0].shape[0]
    normed = [norm_rows(rep).astype(BF16) for rep in reps]
    for half in range(0, len(reps), 2):
        pieces = project_rows(weights_ref[...], normed[half : half + 2])
        for n, piece in enumerate(pieces):
            p = [piece[k * channels : (k + 1) * channels] for k in range(5)]
            at = first + half + n
            rows = pl.ds(pl.multiple_of(at * channels, channels), channels)
            mask = masks[half + n]
            scratch[0, rows, :] = mask * sigmoid(p[0]) * p[1]
            scratch[1, rows, :] = mask * sigmoid(p[2]) * p[3]
            gate_ref[at] = sigmoid(p[4]).astype(gate_ref.dtype)


def store_by_channel(scratch, pair_ref):
    slots, _, per_slot = pair_ref.shape[:3]
    channels = slots * per_slot
    for side in range(2):
        for channel in range(channels):
            rows = scratch[side, pl.ds(channel, GROUP, stride=channels), :]
            pair_ref[channel // per_slot, side, channel % per_slot] = rows.astype(BF16)


STEP = 4


def block_mask(counts_ref, width, unit):
    template = lax.axis_index("tmpl")
    lanes = lax.broadcasted_iota(jnp.int32, (1, width), 1)
    owners = width // unit
    first = lax.axis_index("col") * owners
    mask = jnp.zeros((1, width), F32)
    for owner in range(owners):
        low = owner * unit
        inside = (lanes >= low) & (lanes < low + counts_ref[template, first + owner])
        mask = jnp.where(inside, 1.0, mask)
    return mask


def selection(cover, unit):
    width = cover.shape[1]
    source = lax.broadcasted_iota(jnp.int32, (width, width), 0)
    target = lax.broadcasted_iota(jnp.int32, (width, width), 1)
    upper = ((source <= target) & (source // unit == target // unit)).astype(F32).astype(BF16)
    wide = jnp.broadcast_to(cover, (GROUP, width)).astype(BF16)
    ranks = jnp.dot(wide, upper, preferred_element_type=F32)[:1].astype(jnp.int32)
    slots = target[:1] // unit * unit + ranks - 1
    return jnp.where((source == slots) & (cover > 0.5), 1.0, 0.0)


def template_row(rows, template):
    out = rows[:1]
    for t in range(1, rows.shape[0]):
        out = jnp.where(template == t, rows[t : t + 1], out)
    return out


def pre_kernel(unit, cover_ref, chain_ref, counts_ref, tp_hbm, trunk_hbm, cover_all_ref, chain_all_ref, chain_vec_ref,
               trunk_weights_ref, weights_ref, pair_ref, rep_ref, gate_ref,
               scratch, tp_buffer, trunk_buffer, order, pick, sems):
    step_id = pl.program_id(0)
    base = step_id * GROUP
    cols = tp_buffer.shape[3]
    channels = tp_buffer.shape[2]
    template = lax.axis_index("tmpl")
    row_start = lax.axis_index("row") * unit
    col_start = pl.multiple_of(lax.axis_index("col") * cols, cols)
    slot = lax.rem(step_id, 2)

    def copies(group, into):
        out = []
        for n in range(GROUP):
            row = order[group * GROUP + n]
            out.append(pltpu.make_async_copy(tp_hbm.at[0, row], tp_buffer.at[into, n], sems.at[into, 0, n]))
            out.append(pltpu.make_async_copy(trunk_hbm.at[row], trunk_buffer.at[into, n], sems.at[into, 1, n]))
        return out

    @pl.when(step_id == 0)
    def _():
        def place(row, taken):
            covered = cover_ref[template, row_start + row]
            order[jnp.where(covered > 0, taken, unit - 1 - (row - taken))] = row
            return taken + covered

        lax.fori_loop(0, unit, place, 0)
        for copy in copies(0, 0):
            copy.start()
        cover = template_row(cover_all_ref[:, pl.ds(col_start, cols)].astype(F32), template)
        pick[...] = jnp.transpose(selection(cover, unit)).astype(BF16)

    @pl.when(step_id + 1 < pl.num_programs(0))
    def _():
        for copy in copies(step_id + 1, 1 - slot):
            copy.start()

    for copy in copies(step_id, slot):
        copy.wait()

    trunk_weights = trunk_weights_ref[...]
    weight_sums = jnp.sum(trunk_weights.astype(F32), axis=1, keepdims=True)
    chain_cols = chain_all_ref[:, pl.ds(col_start, cols)]
    col_mask = block_mask(counts_ref, cols, unit)
    row_count = counts_ref[template, lax.axis_index("row")]

    def body(step, carry):
        first = step * STEP
        raw, masks = [], []
        rows = [trunk_buffer[slot, first + n] for n in range(STEP)]
        projected = []
        for half in range(0, STEP, 2):
            projected += project_rows(trunk_weights, rows[half : half + 2])
        for n in range(STEP):
            at = first + n
            values = rows[n].astype(F32)
            scale = 1.0 / values.shape[0]
            centre = jnp.sum(values, axis=0, keepdims=True) * scale
            centred = values - centre
            spread = jnp.sum(centred * centred, axis=0, keepdims=True) * scale
            trunk_proj = (projected[n] - weight_sums * centre) * lax.rsqrt(spread + epsilon)
            same = (chain_cols == chain_ref[row_start + order[base + at]]).astype(F32)
            raw.append((tp_buffer[slot, at].astype(F32) + same * chain_vec_ref[...] + trunk_proj).astype(BF16))
            masks.append(jnp.where(base + at < row_count, col_mask, 0.0))
        picked = jnp.dot(jnp.concatenate(raw, axis=0), pick[...], preferred_element_type=F32)
        reps = [picked[n * channels : (n + 1) * channels] for n in range(STEP)]
        for n in range(STEP):
            rep_ref[first + n] = reps[n].astype(BF16)
        emit_gated(reps, masks, first, weights_ref, gate_ref, scratch)
        return carry

    lax.fori_loop(0, GROUP // STEP, body, 0)
    store_by_channel(scratch, pair_ref)


def load_tri(tri_ref, tri_scratch):
    channels = tri_ref.shape[0]
    scale = 1.0 / channels
    half = GROUP // 2
    for part in range(2):
        rows = slice(part * half, (part + 1) * half)
        total = jnp.zeros((half, tri_ref.shape[2]), F32)
        for channel in range(channels):
            total += tri_ref[channel].astype(F32)[rows]
        centre = total * scale
        total = jnp.zeros_like(total)
        for channel in range(channels):
            centred = tri_ref[channel].astype(F32)[rows] - centre
            total += centred * centred
        inverse = lax.rsqrt(total * scale + epsilon)
        for channel in range(channels):
            tri_scratch[channel * GROUP + part * half : channel * GROUP + (part + 1) * half, :] = (
                tri_ref[channel].astype(F32)[rows] - centre
            ) * inverse


def updated_rows(first, tri_scratch, rep_ref, gate_ref, out_weights_ref):
    channels = rep_ref.shape[1]
    normed = [
        tri_scratch[pl.ds(first + n, channels, stride=GROUP), :].astype(BF16) for n in range(STEP)
    ]
    projected = []
    for half in range(0, STEP, 2):
        projected += project_rows(out_weights_ref[...], normed[half : half + 2])
    return [
        (rep_ref[first + n].astype(F32) + gate_ref[first + n].astype(F32) * projected[n]).astype(BF16)
        for n in range(STEP)
    ]


def mid_kernel(unit, counts_ref, tri_ref, rep_in_ref, gate_in_ref, out_weights_ref, weights_ref,
               pair_ref, rep_ref, gate_ref, scratch, tri_scratch):
    base = pl.program_id(0) * GROUP
    load_tri(tri_ref, tri_scratch)
    col_mask = block_mask(counts_ref, rep_ref.shape[2], unit)
    row_count = counts_ref[lax.axis_index("tmpl"), lax.axis_index("row")]

    def body(step, carry):
        first = step * STEP
        rows = updated_rows(first, tri_scratch, rep_in_ref, gate_in_ref, out_weights_ref)
        masks = []
        for n in range(STEP):
            rep_ref[first + n] = rows[n]
            masks.append(jnp.where(base + first + n < row_count, col_mask, 0.0))
        emit_gated([row.astype(F32) for row in rows], masks, first, weights_ref, gate_ref, scratch)
        return carry

    lax.fori_loop(0, GROUP // STEP, body, 0)
    store_by_channel(scratch, pair_ref)


def last_kernel(tri_ref, rep_in_ref, gate_in_ref, out_weights_ref, pooled_ref, tri_scratch):
    load_tri(tri_ref, tri_scratch)

    def body(step, carry):
        first = step * STEP
        rows = updated_rows(first, tri_scratch, rep_in_ref, gate_in_ref, out_weights_ref)
        for n in range(STEP):
            pooled_ref[first + n] = norm_rows(rows[n].astype(F32)).astype(BF16)
        return carry

    lax.fori_loop(0, GROUP // STEP, body, 0)


def finish_kernel(unit, cover_ref, mine_ref, other_ref, trunk_ref, cover_all_ref, final_weights_ref, out_ref,
                  place, spread):
    step_id = pl.program_id(0)
    base = step_id * GROUP
    cols = out_ref.shape[2]
    channels = mine_ref.shape[1]
    template = lax.axis_index("tmpl")
    templates = (template, 1 - template)
    row_start = lax.axis_index("row") * unit
    col_start = pl.multiple_of(lax.axis_index("col") * cols, cols)
    cover_cols = cover_all_ref[:, pl.ds(col_start, cols)].astype(F32)
    covers = [template_row(cover_cols, t) for t in templates]

    @pl.when(step_id == 0)
    def _():
        for k, t in enumerate(templates):

            def count(row, taken, k=k, t=t):
                covered = cover_ref[t, row_start + row]
                place[k, row] = jnp.where(covered > 0, taken, 0)
                return taken + covered

            lax.fori_loop(0, unit, count, 0)
            spread[k * cols : (k + 1) * cols, :] = selection(covers[k], unit).astype(BF16)

    def body(step, carry):
        first = step * STEP
        packed, counts = [], []
        for n in range(STEP):
            row = base + first + n
            parts = []
            count = jnp.zeros_like(covers[0])
            for k, (t, ref) in enumerate(zip(templates, (mine_ref, other_ref))):
                covered = cover_ref[t, row_start + row]
                value = ref[place[k, row]].astype(F32)
                parts.append(jnp.where(covered > 0, value, 0.0).astype(BF16))
                count += covers[k] * covered.astype(F32)
            packed.append(jnp.concatenate(parts, axis=1))
            counts.append(count)
        pooled = jnp.dot(jnp.concatenate(packed, axis=0), spread[...], preferred_element_type=F32)
        hidden = [
            jnp.maximum(pooled[n * channels : (n + 1) * channels] / jnp.maximum(counts[n], 1.0), 0.0).astype(BF16)
            for n in range(STEP)
        ]
        for half in range(0, STEP, 2):
            for n, row in enumerate(project_rows(final_weights_ref[...], hidden[half : half + 2])):
                at = first + half + n
                out_ref[at] = (trunk_ref[at].astype(F32) + row).astype(BF16)
        return carry

    lax.fori_loop(0, GROUP // STEP, body, 0)


def gather_sides(rows_n, cols_n, unit, pair_ref, sides):
    height, width = pair_ref.shape[3:]

    @pl.when(pl.program_id(0) == 0)
    def _():
        if height < unit:
            sides[...] = jnp.zeros_like(sides)

    for side in range(2):
        for r in range(rows_n):
            for c in range(cols_n):
                sides[side, r * unit : r * unit + height, c * width : (c + 1) * width] = pair_ref[
                    r * cols_n + c, side, 0
                ]


def triangle_kernel(contract, rows_n, cols_n, unit, pair_ref, tri_ref, sides):
    gather_sides(rows_n, cols_n, unit, pair_ref, sides)
    out = lax.dot_general(
        sides[0], sides[1], (((contract,), (contract,)), ((), ())), preferred_element_type=F32
    )
    height, width = tri_ref.shape[2:]
    for r in range(rows_n):
        for c in range(cols_n):
            tri_ref[r * cols_n + c, 0] = out[
                r * unit : r * unit + height, c * width : (c + 1) * width
            ].astype(BF16)


def triangle(contract, rows_n, cols_n, unit, pairs, name):
    slots, _, per_slot, height, width = pairs.shape
    return pl.pallas_call(
        functools.partial(triangle_kernel, contract, rows_n, cols_n, unit),
        grid=(per_slot,),
        in_specs=[pl.BlockSpec((slots, 2, 1, height, width), lambda c: (0, 0, c, 0, 0))],
        out_specs=pl.BlockSpec((slots, 1, height, width), lambda c: (0, c, 0, 0)),
        out_shape=jax.ShapeDtypeStruct((slots, per_slot, height, width), BF16),
        scratch_shapes=[pltpu.VMEM((2, rows_n * unit, cols_n * width), BF16)],
        name=name,
    )(pairs)


SMEM = pl.BlockSpec(memory_space=pltpu.SMEM)
ANY = pl.BlockSpec(memory_space=pl.ANY)


def whole_block(array):
    zeros = (0,) * array.ndim
    return pl.BlockSpec(array.shape, lambda g: zeros)


def rows_block(*rest):
    zeros = (0,) * len(rest)
    return pl.BlockSpec((GROUP,) + rest, lambda g: (g,) + zeros)


def with_capacity(
    capacity,
    counts,
    template_pair,
    trunk,
    coverage,
    chain_ids,
    chain_vec,
    trunk_weights,
    proj_weights,
    out_weights,
    final_weights,
):
    unit, trunk_channels, tile_cols = trunk.shape
    channels = template_pair.shape[2]
    rows_n, cols_n = lax.axis_size("row"), lax.axis_size("col")
    slots = rows_n * cols_n
    per_slot = channels // slots
    grid = (pl.cdiv(capacity, GROUP),)
    stacked = proj_weights.reshape(2, 5 * channels, channels)
    chain_all = chain_ids[None]
    chain_column = chain_vec[:, None]

    pair_spec = pl.BlockSpec((slots, 2, per_slot, GROUP, tile_cols), lambda g: (0, 0, 0, g, 0))
    pair_shape = jax.ShapeDtypeStruct((slots, 2, per_slot, capacity, tile_cols), BF16)
    rep_spec = rows_block(channels, tile_cols)
    rep_shape = jax.ShapeDtypeStruct((capacity, channels, tile_cols), BF16)
    trunk_spec = rows_block(trunk_channels, tile_cols)
    tri_spec = pl.BlockSpec((channels, GROUP, tile_cols), lambda g: (0, g, 0))
    scratch = pltpu.VMEM((2, GROUP * channels, tile_cols), F32)
    tri_scratch = pltpu.VMEM((channels * GROUP, tile_cols), F32)
    gated_outs = dict(
        out_specs=[pair_spec, rep_spec, rep_spec], out_shape=[pair_shape, rep_shape, rep_shape]
    )

    def exchange(values):
        return lax.all_to_all(values, ("row", "col"), 0, 0, tiled=True)

    pairs, rep, gate = pl.pallas_call(
        functools.partial(pre_kernel, unit),
        grid=grid,
        in_specs=[
            SMEM,
            SMEM,
            SMEM,
            ANY,
            ANY,
            whole_block(coverage),
            whole_block(chain_all),
            whole_block(chain_column),
            whole_block(trunk_weights),
            whole_block(stacked[0]),
        ],
        scratch_shapes=[
            scratch,
            pltpu.VMEM((2, GROUP, channels, tile_cols), BF16),
            pltpu.VMEM((2, GROUP, trunk_channels, tile_cols), BF16),
            pltpu.SMEM((unit,), jnp.int32),
            pltpu.VMEM((tile_cols, tile_cols), BF16),
            pltpu.SemaphoreType.DMA((2, 2, GROUP)),
        ],
        name="pre",
        **gated_outs,
    )(coverage, chain_ids, counts, template_pair, trunk, coverage, chain_all, chain_column, trunk_weights, stacked[0])

    tri = exchange(triangle(1, rows_n, cols_n, unit, exchange(pairs), "outgoing"))
    pairs, rep, gate = pl.pallas_call(
        functools.partial(mid_kernel, unit),
        grid=grid,
        in_specs=[SMEM, tri_spec, rep_spec, rep_spec, whole_block(out_weights[0]), whole_block(stacked[1])],
        scratch_shapes=[scratch, tri_scratch],
        name="mid",
        **gated_outs,
    )(counts, tri.reshape(channels, capacity, tile_cols), rep, gate, out_weights[0], stacked[1])

    tri = exchange(triangle(0, rows_n, cols_n, unit, exchange(pairs), "incoming"))
    pooled = pl.pallas_call(
        last_kernel,
        grid=grid,
        in_specs=[tri_spec, rep_spec, rep_spec, whole_block(out_weights[1])],
        out_specs=rep_spec,
        out_shape=rep_shape,
        scratch_shapes=[tri_scratch],
        name="last",
    )(tri.reshape(channels, capacity, tile_cols), rep, gate, out_weights[1])

    other = lax.ppermute(pooled, "tmpl", [(0, 1), (1, 0)])
    return pl.pallas_call(
        functools.partial(finish_kernel, unit),
        grid=(unit // GROUP,),
        in_specs=[
            SMEM,
            whole_block(pooled),
            whole_block(pooled),
            trunk_spec,
            whole_block(coverage),
            whole_block(final_weights),
        ],
        out_specs=trunk_spec,
        out_shape=jax.ShapeDtypeStruct(trunk.shape, BF16),
        scratch_shapes=[pltpu.SMEM((2, unit), jnp.int32), pltpu.VMEM((2 * tile_cols, tile_cols), BF16)],
        name="finish",
    )(coverage, pooled, other, trunk, coverage, final_weights)


def per_device(template_pair, trunk, coverage, *rest):
    unit, _, tile_cols = trunk.shape
    templates, tokens = coverage.shape
    counts = jnp.sum(coverage.reshape(templates, tokens // unit, unit), axis=2)
    capacities = [unit]
    if unit == tile_cols and unit % 16 == 0:
        capacities = [unit * share // 16 for share in (12, 13, 14, 16)]
    args = (counts, template_pair, trunk, coverage) + rest
    if len(capacities) == 1:
        return with_capacity(unit, *args)
    most = jnp.max(counts)
    branch = sum((most > capacity).astype(jnp.int32) for capacity in capacities[:-1])
    return lax.switch(branch, [functools.partial(with_capacity, capacity) for capacity in capacities], *args)


def solution(mesh):
    in_specs = (
        P("tmpl", "row", None, "col"),
        P("row", None, "col"),
        P(),
        P(),
        P(),
        P(),
        P(),
        P(),
        P(),
    )
    out_specs = P("row", None, "col")
    return jax.shard_map(
        per_device, mesh=mesh, in_specs=in_specs, out_specs=out_specs, check_vma=False
    )
```

```python
import functools

import jax
import jax.numpy as jnp
from jax import lax
from jax.experimental import pallas as pl
from jax.experimental.pallas import tpu as pltpu
from jax.sharding import PartitionSpec as P

epsilon = 1e-05
GROUP = 16
F32 = jnp.float32
BF16 = jnp.bfloat16


def sigmoid(x):
    return 0.5 * jnp.tanh(0.5 * x) + 0.5


def norm_rows(x):
    scale = 1.0 / x.shape[0]
    centred = x - jnp.sum(x, axis=0, keepdims=True) * scale
    spread = jnp.sum(centred * centred, axis=0, keepdims=True) * scale
    return centred * lax.rsqrt(spread + epsilon)


def project_rows(weights, rows):
    wide = jnp.concatenate(rows, axis=1)
    out = jnp.dot(weights, wide, preferred_element_type=F32)
    cols = rows[0].shape[1]
    return [out[:, n * cols : (n + 1) * cols] for n in range(len(rows))]


def emit_gated(reps, masks, first, weights_ref, gate_ref, scratch):
    channels = reps[0].shape[0]
    normed = [norm_rows(rep).astype(BF16) for rep in reps]
    for half in range(0, len(reps), 2):
        pieces = project_rows(weights_ref[...], normed[half : half + 2])
        for n, piece in enumerate(pieces):
            p = [piece[k * channels : (k + 1) * channels] for k in range(5)]
            at = first + half + n
            rows = pl.ds(pl.multiple_of(at * (channels + PAD), 8), channels)
            mask = masks[half + n]
            scratch[0, rows, :] = mask * sigmoid(p[0]) * p[1]
            scratch[1, rows, :] = mask * sigmoid(p[2]) * p[3]
            gate_ref[at] = sigmoid(p[4]).astype(gate_ref.dtype)


def store_by_channel(scratch, pair_ref):
    slots, _, per_slot = pair_ref.shape[:3]
    channels = slots * per_slot
    for side in range(2):
        for channel in range(channels):
            rows = scratch[side, pl.ds(channel, GROUP, stride=channels + PAD), :]
            pair_ref[channel // per_slot, side, channel % per_slot] = rows.astype(BF16)


STEP = 16
PAD = 8


def block_mask(counts_ref, width, unit):
    template = lax.axis_index("tmpl")
    lanes = lax.broadcasted_iota(jnp.int32, (1, width), 1)
    owners = width // unit
    first = lax.axis_index("col") * owners
    mask = jnp.zeros((1, width), F32)
    for owner in range(owners):
        low = owner * unit
        inside = (lanes >= low) & (lanes < low + counts_ref[template, first + owner])
        mask = jnp.where(inside, 1.0, mask)
    return mask


def selection(cover, unit):
    width = cover.shape[1]
    source = lax.broadcasted_iota(jnp.int32, (width, width), 0)
    target = lax.broadcasted_iota(jnp.int32, (width, width), 1)
    upper = ((source <= target) & (source // unit == target // unit)).astype(F32).astype(BF16)
    wide = jnp.broadcast_to(cover, (GROUP, width)).astype(BF16)
    ranks = jnp.dot(wide, upper, preferred_element_type=F32)[:1].astype(jnp.int32)
    slots = target[:1] // unit * unit + ranks - 1
    return jnp.where((source == slots) & (cover > 0.5), 1.0, 0.0)


def template_row(rows, template):
    out = rows[:1]
    for t in range(1, rows.shape[0]):
        out = jnp.where(template == t, rows[t : t + 1], out)
    return out


def pre_kernel(unit, cover_ref, chain_ref, counts_ref, tp_hbm, trunk_hbm, cover_all_ref, chain_all_ref, chain_vec_ref,
               trunk_weights_ref, weights_ref, pair_ref, rep_ref, gate_ref,
               scratch, tp_buffer, trunk_buffer, order, pick, sems):
    step_id = pl.program_id(0)
    base = step_id * GROUP
    cols = tp_buffer.shape[3]
    channels = tp_buffer.shape[2]
    template = lax.axis_index("tmpl")
    row_start = lax.axis_index("row") * unit
    col_start = pl.multiple_of(lax.axis_index("col") * cols, cols)
    slot = lax.rem(step_id, 2)

    def copies(group, into):
        out = []
        for n in range(GROUP):
            row = order[group * GROUP + n]
            out.append(pltpu.make_async_copy(tp_hbm.at[0, row], tp_buffer.at[into, n], sems.at[into, 0, n]))
            out.append(pltpu.make_async_copy(trunk_hbm.at[row], trunk_buffer.at[into, n], sems.at[into, 1, n]))
        return out

    @pl.when(step_id == 0)
    def _():
        def place(row, taken):
            covered = cover_ref[template, row_start + row]
            order[jnp.where(covered > 0, taken, unit - 1 - (row - taken))] = row
            return taken + covered

        lax.fori_loop(0, unit, place, 0, unroll=8)
        for copy in copies(0, 0):
            copy.start()
        cover = template_row(cover_all_ref[:, pl.ds(col_start, cols)].astype(F32), template)
        pick[...] = jnp.transpose(selection(cover, unit)).astype(BF16)

    @pl.when(step_id + 1 < pl.num_programs(0))
    def _():
        for copy in copies(step_id + 1, 1 - slot):
            copy.start()

    for copy in copies(step_id, slot):
        copy.wait()

    trunk_weights = trunk_weights_ref[...]
    weight_sums = jnp.sum(trunk_weights.astype(F32), axis=1, keepdims=True)
    chain_cols = chain_all_ref[:, pl.ds(col_start, cols)]
    col_mask = block_mask(counts_ref, cols, unit)
    row_count = counts_ref[template, lax.axis_index("row")]

    def body(step, carry):
        first = step * STEP
        raw, masks = [], []
        rows = [trunk_buffer[slot, first + n] for n in range(STEP)]
        projected = []
        for half in range(0, STEP, 2):
            projected += project_rows(trunk_weights, rows[half : half + 2])
        for n in range(STEP):
            at = first + n
            values = rows[n].astype(F32)
            scale = 1.0 / values.shape[0]
            centre = jnp.sum(values, axis=0, keepdims=True) * scale
            centred = values - centre
            spread = jnp.sum(centred * centred, axis=0, keepdims=True) * scale
            trunk_proj = (projected[n] - weight_sums * centre) * lax.rsqrt(spread + epsilon)
            same = (chain_cols == chain_ref[row_start + order[base + at]]).astype(F32)
            raw.append((tp_buffer[slot, at].astype(F32) + same * chain_vec_ref[...] + trunk_proj).astype(BF16))
            masks.append(jnp.where(base + at < row_count, col_mask, 0.0))
        picked = jnp.dot(jnp.concatenate(raw, axis=0), pick[...], preferred_element_type=F32)
        reps = [picked[n * channels : (n + 1) * channels] for n in range(STEP)]
        for n in range(STEP):
            rep_ref[first + n] = reps[n].astype(BF16)
        emit_gated(reps, masks, first, weights_ref, gate_ref, scratch)
        return carry

    lax.fori_loop(0, GROUP // STEP, body, 0)
    store_by_channel(scratch, pair_ref)


def load_tri(tri_ref, tri_scratch):
    channels = tri_ref.shape[0]
    scale = 1.0 / channels
    half = GROUP // 2
    for part in range(2):
        rows = slice(part * half, (part + 1) * half)
        total = jnp.zeros((half, tri_ref.shape[2]), F32)
        for channel in range(channels):
            total += tri_ref[channel].astype(F32)[rows]
        centre = total * scale
        total = jnp.zeros_like(total)
        for channel in range(channels):
            centred = tri_ref[channel].astype(F32)[rows] - centre
            total += centred * centred
        inverse = lax.rsqrt(total * scale + epsilon)
        for channel in range(channels):
            at = channel * (GROUP + PAD) + part * half
            tri_scratch[at : at + half, :] = (
                tri_ref[channel].astype(F32)[rows] - centre
            ) * inverse


def updated_rows(first, tri_scratch, rep_ref, gate_ref, out_weights_ref):
    channels = rep_ref.shape[1]
    normed = [
        tri_scratch[pl.ds(first + n, channels, stride=GROUP + PAD), :].astype(BF16) for n in range(STEP)
    ]
    projected = []
    for half in range(0, STEP, 2):
        projected += project_rows(out_weights_ref[...], normed[half : half + 2])
    return [
        (rep_ref[first + n].astype(F32) + gate_ref[first + n].astype(F32) * projected[n]).astype(BF16)
        for n in range(STEP)
    ]


def mid_kernel(unit, counts_ref, tri_ref, rep_in_ref, gate_in_ref, out_weights_ref, weights_ref,
               pair_ref, rep_ref, gate_ref, scratch, tri_scratch):
    base = pl.program_id(0) * GROUP
    load_tri(tri_ref, tri_scratch)
    col_mask = block_mask(counts_ref, rep_ref.shape[2], unit)
    row_count = counts_ref[lax.axis_index("tmpl"), lax.axis_index("row")]

    def body(step, carry):
        first = step * STEP
        rows = updated_rows(first, tri_scratch, rep_in_ref, gate_in_ref, out_weights_ref)
        masks = []
        for n in range(STEP):
            rep_ref[first + n] = rows[n]
            masks.append(jnp.where(base + first + n < row_count, col_mask, 0.0))
        emit_gated([row.astype(F32) for row in rows], masks, first, weights_ref, gate_ref, scratch)
        return carry

    lax.fori_loop(0, GROUP // STEP, body, 0)
    store_by_channel(scratch, pair_ref)


def last_kernel(tri_ref, rep_in_ref, gate_in_ref, out_weights_ref, pooled_ref, tri_scratch):
    load_tri(tri_ref, tri_scratch)

    def body(step, carry):
        first = step * STEP
        rows = updated_rows(first, tri_scratch, rep_in_ref, gate_in_ref, out_weights_ref)
        for n in range(STEP):
            pooled_ref[first + n] = norm_rows(rows[n].astype(F32)).astype(BF16)
        return carry

    lax.fori_loop(0, GROUP // STEP, body, 0)


def finish_kernel(unit, cover_ref, mine_ref, other_ref, trunk_ref, cover_all_ref, final_weights_ref, out_ref,
                  place, spread):
    step_id = pl.program_id(0)
    base = step_id * GROUP
    cols = out_ref.shape[2]
    channels = mine_ref.shape[1]
    template = lax.axis_index("tmpl")
    templates = (template, 1 - template)
    row_start = lax.axis_index("row") * unit
    col_start = pl.multiple_of(lax.axis_index("col") * cols, cols)
    cover_cols = cover_all_ref[:, pl.ds(col_start, cols)].astype(F32)
    covers = [template_row(cover_cols, t) for t in templates]

    @pl.when(step_id == 0)
    def _():
        def count(row, taken):
            out = []
            for k, t in enumerate(templates):
                covered = cover_ref[t, row_start + row]
                place[k, row] = jnp.where(covered > 0, taken[k], 0)
                out.append(taken[k] + covered)
            return tuple(out)

        lax.fori_loop(0, unit, count, (0,) * len(templates), unroll=8)
        for k in range(len(templates)):
            spread[k * cols : (k + 1) * cols, :] = selection(covers[k], unit).astype(BF16)

    def body(step, carry):
        first = step * STEP
        packed, counts = [], []
        for n in range(STEP):
            row = base + first + n
            parts = []
            count = jnp.zeros_like(covers[0])
            for k, (t, ref) in enumerate(zip(templates, (mine_ref, other_ref))):
                covered = cover_ref[t, row_start + row]
                value = ref[place[k, row]].astype(F32)
                parts.append(jnp.where(covered > 0, value, 0.0).astype(BF16))
                count += covers[k] * covered.astype(F32)
            packed.append(jnp.concatenate(parts, axis=1))
            counts.append(count)
        pooled = jnp.dot(jnp.concatenate(packed, axis=0), spread[...], preferred_element_type=F32)
        hidden = [
            jnp.maximum(pooled[n * channels : (n + 1) * channels] * (1.0 / jnp.maximum(counts[n], 1.0)), 0.0).astype(BF16)
            for n in range(STEP)
        ]
        for half in range(0, STEP, 2):
            for n, row in enumerate(project_rows(final_weights_ref[...], hidden[half : half + 2])):
                at = first + half + n
                out_ref[at] = (trunk_ref[at].astype(F32) + row).astype(BF16)
        return carry

    lax.fori_loop(0, GROUP // STEP, body, 0)


def gather_sides(rows_n, cols_n, unit, pair_ref, sides):
    height, width = pair_ref.shape[3:]

    @pl.when(pl.program_id(0) == 0)
    def _():
        if height < unit:
            sides[...] = jnp.zeros_like(sides)

    for side in range(2):
        for r in range(rows_n):
            for c in range(cols_n):
                sides[side, r * unit : r * unit + height, c * width : (c + 1) * width] = pair_ref[
                    r * cols_n + c, side, 0
                ]


def triangle_kernel(contract, rows_n, cols_n, unit, pair_ref, tri_ref, sides):
    gather_sides(rows_n, cols_n, unit, pair_ref, sides)
    out = lax.dot_general(
        sides[0], sides[1], (((contract,), (contract,)), ((), ())), preferred_element_type=F32
    )
    height, width = tri_ref.shape[2:]
    for r in range(rows_n):
        for c in range(cols_n):
            tri_ref[r * cols_n + c, 0] = out[
                r * unit : r * unit + height, c * width : (c + 1) * width
            ].astype(BF16)


def triangle(contract, rows_n, cols_n, unit, pairs, name):
    slots, _, per_slot, height, width = pairs.shape
    return pl.pallas_call(
        functools.partial(triangle_kernel, contract, rows_n, cols_n, unit),
        grid=(per_slot,),
        in_specs=[pl.BlockSpec((slots, 2, 1, height, width), lambda c: (0, 0, c, 0, 0))],
        out_specs=pl.BlockSpec((slots, 1, height, width), lambda c: (0, c, 0, 0)),
        out_shape=jax.ShapeDtypeStruct((slots, per_slot, height, width), BF16),
        scratch_shapes=[pltpu.VMEM((2, rows_n * unit, cols_n * width), BF16)],
        name=name,
    )(pairs)


SMEM = pl.BlockSpec(memory_space=pltpu.SMEM)
ANY = pl.BlockSpec(memory_space=pl.ANY)


def whole_block(array):
    zeros = (0,) * array.ndim
    return pl.BlockSpec(array.shape, lambda g: zeros)


def rows_block(*rest):
    zeros = (0,) * len(rest)
    return pl.BlockSpec((GROUP,) + rest, lambda g: (g,) + zeros)


def with_capacity(
    capacity,
    counts,
    template_pair,
    trunk,
    coverage,
    chain_ids,
    chain_vec,
    trunk_weights,
    proj_weights,
    out_weights,
    final_weights,
):
    unit, trunk_channels, tile_cols = trunk.shape
    channels = template_pair.shape[2]
    rows_n, cols_n = lax.axis_size("row"), lax.axis_size("col")
    slots = rows_n * cols_n
    per_slot = channels // slots
    grid = (pl.cdiv(capacity, GROUP),)
    stacked = proj_weights.reshape(2, 5 * channels, channels)
    chain_all = chain_ids[None]
    chain_column = chain_vec[:, None]

    pair_spec = pl.BlockSpec((slots, 2, per_slot, GROUP, tile_cols), lambda g: (0, 0, 0, g, 0))
    pair_shape = jax.ShapeDtypeStruct((slots, 2, per_slot, capacity, tile_cols), BF16)
    rep_spec = rows_block(channels, tile_cols)
    rep_shape = jax.ShapeDtypeStruct((capacity, channels, tile_cols), BF16)
    trunk_spec = rows_block(trunk_channels, tile_cols)
    tri_spec = pl.BlockSpec((channels, GROUP, tile_cols), lambda g: (0, g, 0))
    scratch = pltpu.VMEM((2, GROUP * (channels + PAD), tile_cols), F32)
    tri_scratch = pltpu.VMEM((channels * (GROUP + PAD), tile_cols), F32)
    gated_outs = dict(
        out_specs=[pair_spec, rep_spec, rep_spec], out_shape=[pair_shape, rep_shape, rep_shape]
    )

    def exchange(values):
        return lax.all_to_all(values, ("row", "col"), 0, 0, tiled=True)

    pairs, rep, gate = pl.pallas_call(
        functools.partial(pre_kernel, unit),
        grid=grid,
        in_specs=[
            SMEM,
            SMEM,
            SMEM,
            ANY,
            ANY,
            whole_block(coverage),
            whole_block(chain_all),
            whole_block(chain_column),
            whole_block(trunk_weights),
            whole_block(stacked[0]),
        ],
        scratch_shapes=[
            scratch,
            pltpu.VMEM((2, GROUP, channels, tile_cols), BF16),
            pltpu.VMEM((2, GROUP, trunk_channels, tile_cols), BF16),
            pltpu.SMEM((unit,), jnp.int32),
            pltpu.VMEM((tile_cols, tile_cols), BF16),
            pltpu.SemaphoreType.DMA((2, 2, GROUP)),
        ],
        name="pre",
        **gated_outs,
    )(coverage, chain_ids, counts, template_pair, trunk, coverage, chain_all, chain_column, trunk_weights, stacked[0])

    tri = exchange(triangle(1, rows_n, cols_n, unit, exchange(pairs), "outgoing"))
    pairs, rep, gate = pl.pallas_call(
        functools.partial(mid_kernel, unit),
        grid=grid,
        in_specs=[SMEM, tri_spec, rep_spec, rep_spec, whole_block(out_weights[0]), whole_block(stacked[1])],
        scratch_shapes=[scratch, tri_scratch],
        name="mid",
        **gated_outs,
    )(counts, tri.reshape(channels, capacity, tile_cols), rep, gate, out_weights[0], stacked[1])

    tri = exchange(triangle(0, rows_n, cols_n, unit, exchange(pairs), "incoming"))
    pooled = pl.pallas_call(
        last_kernel,
        grid=grid,
        in_specs=[tri_spec, rep_spec, rep_spec, whole_block(out_weights[1])],
        out_specs=rep_spec,
        out_shape=rep_shape,
        scratch_shapes=[tri_scratch],
        name="last",
    )(tri.reshape(channels, capacity, tile_cols), rep, gate, out_weights[1])

    other = lax.ppermute(pooled, "tmpl", [(0, 1), (1, 0)])
    return pl.pallas_call(
        functools.partial(finish_kernel, unit),
        grid=(unit // GROUP,),
        in_specs=[
            SMEM,
            whole_block(pooled),
            whole_block(pooled),
            trunk_spec,
            whole_block(coverage),
            whole_block(final_weights),
        ],
        out_specs=trunk_spec,
        out_shape=jax.ShapeDtypeStruct(trunk.shape, BF16),
        scratch_shapes=[pltpu.SMEM((2, unit), jnp.int32), pltpu.VMEM((2 * tile_cols, tile_cols), BF16)],
        name="finish",
    )(coverage, pooled, other, trunk, coverage, final_weights)


def per_device(template_pair, trunk, coverage, *rest):
    unit, _, tile_cols = trunk.shape
    templates, tokens = coverage.shape
    counts = jnp.sum(coverage.reshape(templates, tokens // unit, unit), axis=2)
    capacities = [unit]
    if unit == tile_cols and unit % 16 == 0:
        capacities = [unit * share // 16 for share in (12, 13, 14, 16)]
    args = (counts, template_pair, trunk, coverage) + rest
    if len(capacities) == 1:
        return with_capacity(unit, *args)
    most = jnp.max(counts)
    branch = sum((most > capacity).astype(jnp.int32) for capacity in capacities[:-1])
    return lax.switch(branch, [functools.partial(with_capacity, capacity) for capacity in capacities], *args)


def solution(mesh):
    in_specs = (
        P("tmpl", "row", None, "col"),
        P("row", None, "col"),
        P(),
        P(),
        P(),
        P(),
        P(),
        P(),
        P(),
    )
    out_specs = P("row", None, "col")
    return jax.shard_map(
        per_device, mesh=mesh, in_specs=in_specs, out_specs=out_specs, check_vma=False
    )
```

```python
import functools

import jax
import jax.numpy as jnp
from jax import lax
from jax.experimental import pallas as pl
from jax.experimental.pallas import tpu as pltpu
from jax.sharding import PartitionSpec as P

epsilon = 1e-05
GROUP = 16
F32 = jnp.float32
BF16 = jnp.bfloat16


def sigmoid(x):
    return 0.5 * jnp.tanh(0.5 * x) + 0.5


def norm_rows(x):
    scale = 1.0 / x.shape[0]
    centred = x - jnp.sum(x, axis=0, keepdims=True) * scale
    spread = jnp.sum(centred * centred, axis=0, keepdims=True) * scale
    return centred * lax.rsqrt(spread + epsilon)


def project_rows(weights, rows):
    wide = jnp.concatenate(rows, axis=1)
    out = jnp.dot(weights, wide, preferred_element_type=F32)
    cols = rows[0].shape[1]
    return [out[:, n * cols : (n + 1) * cols] for n in range(len(rows))]


def emit_gated(reps, masks, first, weights_ref, gate_ref, scratch):
    channels = reps[0].shape[0]
    normed = [norm_rows(rep).astype(BF16) for rep in reps]
    for half in range(0, len(reps), 2):
        pieces = project_rows(weights_ref[...], normed[half : half + 2])
        for n, piece in enumerate(pieces):
            p = [piece[k * channels : (k + 1) * channels] for k in range(5)]
            at = first + half + n
            rows = pl.ds(pl.multiple_of(at * (channels + PAD), 8), channels)
            mask = masks[half + n]
            scratch[0, rows, :] = mask * sigmoid(p[0]) * p[1]
            scratch[1, rows, :] = mask * sigmoid(p[2]) * p[3]
            gate_ref[at] = sigmoid(p[4]).astype(gate_ref.dtype)


def packing(capacity, unit, width, per_slot):
    if unit == width:
        for q, p in ((4, 3), (8, 7)):
            if capacity * q <= width * p and 2 * per_slot % q == 0:
                return q, p
    return 1, 1


def lanes_of(shape, dtype=jnp.int32):
    return lax.broadcasted_iota(dtype, shape, len(shape) - 1)


def pack(units, q, p):
    if q == 1:
        return units
    width = units[0].shape[-1]
    kept, piece = width // q * p, width // q
    free = lanes_of(units[0].shape) >= kept
    out = []
    for first in range(0, len(units), q):
        last = units[first + q - 1]
        for e in range(p):
            out.append(jnp.where(free, pltpu.roll(last, kept - e * piece, 1), units[first + e]))
    return out


def unpack_last(packed, q, p):
    width = packed[0].shape[-1]
    piece = width // q
    at = lanes_of(packed[0].shape) // piece
    out = jnp.zeros_like(packed[0])
    for e in range(p):
        out = jnp.where(at == e, pltpu.roll(packed[e], (e + 1) * piece, 1), out)
    return out


def store_by_channel(q, p, scratch, pair_ref):
    slots, units = pair_ref.shape[:2]
    per_slot = units // p * q // 2
    channels = slots * per_slot
    for slot in range(slots):
        values = [
            scratch[side, pl.ds(slot * per_slot + channel, GROUP, stride=channels + PAD), :]
            for side in range(2)
            for channel in range(per_slot)
        ]
        for n, value in enumerate(pack(values, q, p)):
            pair_ref[slot, n] = value.astype(BF16)


STEP = 16
PAD = 8


def block_mask(counts_ref, width, unit):
    template = lax.axis_index("tmpl")
    lanes = lax.broadcasted_iota(jnp.int32, (1, width), 1)
    owners = width // unit
    first = lax.axis_index("col") * owners
    mask = jnp.zeros((1, width), F32)
    for owner in range(owners):
        low = owner * unit
        inside = (lanes >= low) & (lanes < low + counts_ref[template, first + owner])
        mask = jnp.where(inside, 1.0, mask)
    return mask


def selection(cover, unit):
    width = cover.shape[1]
    source = lax.broadcasted_iota(jnp.int32, (width, width), 0)
    target = lax.broadcasted_iota(jnp.int32, (width, width), 1)
    upper = ((source <= target) & (source // unit == target // unit)).astype(F32).astype(BF16)
    wide = jnp.broadcast_to(cover, (GROUP, width)).astype(BF16)
    ranks = jnp.dot(wide, upper, preferred_element_type=F32)[:1].astype(jnp.int32)
    slots = target[:1] // unit * unit + ranks - 1
    return jnp.where((source == slots) & (cover > 0.5), 1.0, 0.0)


def template_row(rows, template):
    out = rows[:1]
    for t in range(1, rows.shape[0]):
        out = jnp.where(template == t, rows[t : t + 1], out)
    return out


def pre_kernel(unit, q, p, cover_ref, chain_ref, counts_ref, tp_hbm, trunk_hbm, cover_all_ref, chain_all_ref, chain_vec_ref,
               trunk_weights_ref, weights_ref, pair_ref, rep_ref, gate_ref,
               scratch, tp_buffer, trunk_buffer, order, pick, sems):
    step_id = pl.program_id(0)
    base = step_id * GROUP
    cols = tp_buffer.shape[3]
    channels = tp_buffer.shape[2]
    template = lax.axis_index("tmpl")
    row_start = lax.axis_index("row") * unit
    col_start = pl.multiple_of(lax.axis_index("col") * cols, cols)
    slot = lax.rem(step_id, 2)

    def copies(group, into):
        out = []
        for n in range(GROUP):
            row = order[group * GROUP + n]
            out.append(pltpu.make_async_copy(tp_hbm.at[0, row], tp_buffer.at[into, n], sems.at[into, 0, n]))
            out.append(pltpu.make_async_copy(trunk_hbm.at[row], trunk_buffer.at[into, n], sems.at[into, 1, n]))
        return out

    @pl.when(step_id == 0)
    def _():
        def place(row, taken):
            covered = cover_ref[template, row_start + row]
            order[jnp.where(covered > 0, taken, unit - 1 - (row - taken))] = row
            return taken + covered

        lax.fori_loop(0, unit, place, 0, unroll=8)
        for copy in copies(0, 0):
            copy.start()
        cover = template_row(cover_all_ref[:, pl.ds(col_start, cols)].astype(F32), template)
        pick[...] = jnp.transpose(selection(cover, unit)).astype(BF16)

    @pl.when(step_id + 1 < pl.num_programs(0))
    def _():
        for copy in copies(step_id + 1, 1 - slot):
            copy.start()

    for copy in copies(step_id, slot):
        copy.wait()

    trunk_weights = trunk_weights_ref[...]
    weight_sums = jnp.sum(trunk_weights.astype(F32), axis=1, keepdims=True)
    chain_cols = chain_all_ref[:, pl.ds(col_start, cols)]
    col_mask = block_mask(counts_ref, cols, unit)
    row_count = counts_ref[template, lax.axis_index("row")]

    def body(step, carry):
        first = step * STEP
        raw, masks = [], []
        rows = [trunk_buffer[slot, first + n] for n in range(STEP)]
        projected = []
        for half in range(0, STEP, 2):
            projected += project_rows(trunk_weights, rows[half : half + 2])
        for n in range(STEP):
            at = first + n
            values = rows[n].astype(F32)
            scale = 1.0 / values.shape[0]
            centre = jnp.sum(values, axis=0, keepdims=True) * scale
            centred = values - centre
            spread = jnp.sum(centred * centred, axis=0, keepdims=True) * scale
            trunk_proj = (projected[n] - weight_sums * centre) * lax.rsqrt(spread + epsilon)
            same = (chain_cols == chain_ref[row_start + order[base + at]]).astype(F32)
            raw.append((tp_buffer[slot, at].astype(F32) + same * chain_vec_ref[...] + trunk_proj).astype(BF16))
            masks.append(jnp.where(base + at < row_count, col_mask, 0.0))
        picked = jnp.dot(jnp.concatenate(raw, axis=0), pick[...], preferred_element_type=F32)
        reps = [picked[n * channels : (n + 1) * channels] for n in range(STEP)]
        for n in range(STEP):
            rep_ref[first + n] = reps[n].astype(BF16)
        emit_gated(reps, masks, first, weights_ref, gate_ref, scratch)
        return carry

    lax.fori_loop(0, GROUP // STEP, body, 0)
    store_by_channel(q, p, scratch, pair_ref)


def load_tri(tri_ref, tri_scratch):
    channels = tri_ref.shape[0]
    scale = 1.0 / channels
    half = GROUP // 2
    for part in range(2):
        rows = slice(part * half, (part + 1) * half)
        total = jnp.zeros((half, tri_ref.shape[2]), F32)
        for channel in range(channels):
            total += tri_ref[channel].astype(F32)[rows]
        centre = total * scale
        total = jnp.zeros_like(total)
        for channel in range(channels):
            centred = tri_ref[channel].astype(F32)[rows] - centre
            total += centred * centred
        inverse = lax.rsqrt(total * scale + epsilon)
        for channel in range(channels):
            at = channel * (GROUP + PAD) + part * half
            tri_scratch[at : at + half, :] = (
                tri_ref[channel].astype(F32)[rows] - centre
            ) * inverse


def updated_rows(first, tri_scratch, rep_ref, gate_ref, out_weights_ref):
    channels = rep_ref.shape[1]
    normed = [
        tri_scratch[pl.ds(first + n, channels, stride=GROUP + PAD), :].astype(BF16) for n in range(STEP)
    ]
    projected = []
    for half in range(0, STEP, 2):
        projected += project_rows(out_weights_ref[...], normed[half : half + 2])
    return [
        (rep_ref[first + n].astype(F32) + gate_ref[first + n].astype(F32) * projected[n]).astype(BF16)
        for n in range(STEP)
    ]


def mid_kernel(unit, q, p, counts_ref, tri_ref, rep_in_ref, gate_in_ref, out_weights_ref, weights_ref,
               pair_ref, rep_ref, gate_ref, scratch, tri_scratch):
    base = pl.program_id(0) * GROUP
    load_tri(tri_ref, tri_scratch)
    col_mask = block_mask(counts_ref, rep_ref.shape[2], unit)
    row_count = counts_ref[lax.axis_index("tmpl"), lax.axis_index("row")]

    def body(step, carry):
        first = step * STEP
        rows = updated_rows(first, tri_scratch, rep_in_ref, gate_in_ref, out_weights_ref)
        masks = []
        for n in range(STEP):
            rep_ref[first + n] = rows[n]
            masks.append(jnp.where(base + first + n < row_count, col_mask, 0.0))
        emit_gated([row.astype(F32) for row in rows], masks, first, weights_ref, gate_ref, scratch)
        return carry

    lax.fori_loop(0, GROUP // STEP, body, 0)
    store_by_channel(q, p, scratch, pair_ref)


def last_kernel(tri_ref, rep_in_ref, gate_in_ref, out_weights_ref, pooled_ref, tri_scratch):
    load_tri(tri_ref, tri_scratch)

    def body(step, carry):
        first = step * STEP
        rows = updated_rows(first, tri_scratch, rep_in_ref, gate_in_ref, out_weights_ref)
        for n in range(STEP):
            pooled_ref[first + n] = norm_rows(rows[n].astype(F32)).astype(BF16)
        return carry

    lax.fori_loop(0, GROUP // STEP, body, 0)


def finish_kernel(unit, cover_ref, mine_ref, other_ref, trunk_ref, cover_all_ref, final_weights_ref, out_ref,
                  place, spread):
    step_id = pl.program_id(0)
    base = step_id * GROUP
    cols = out_ref.shape[2]
    channels = mine_ref.shape[1]
    template = lax.axis_index("tmpl")
    templates = (template, 1 - template)
    row_start = lax.axis_index("row") * unit
    col_start = pl.multiple_of(lax.axis_index("col") * cols, cols)
    cover_cols = cover_all_ref[:, pl.ds(col_start, cols)].astype(F32)
    covers = [template_row(cover_cols, t) for t in templates]

    @pl.when(step_id == 0)
    def _():
        def count(row, taken):
            out = []
            for k, t in enumerate(templates):
                covered = cover_ref[t, row_start + row]
                place[k, row] = jnp.where(covered > 0, taken[k], 0)
                out.append(taken[k] + covered)
            return tuple(out)

        lax.fori_loop(0, unit, count, (0,) * len(templates), unroll=8)
        for k in range(len(templates)):
            spread[k * cols : (k + 1) * cols, :] = selection(covers[k], unit).astype(BF16)

    def body(step, carry):
        first = step * STEP
        packed, counts = [], []
        for n in range(STEP):
            row = base + first + n
            parts = []
            count = jnp.zeros_like(covers[0])
            for k, (t, ref) in enumerate(zip(templates, (mine_ref, other_ref))):
                covered = cover_ref[t, row_start + row]
                value = ref[place[k, row]].astype(F32)
                parts.append(jnp.where(covered > 0, value, 0.0).astype(BF16))
                count += covers[k] * covered.astype(F32)
            packed.append(jnp.concatenate(parts, axis=1))
            counts.append(count)
        pooled = jnp.dot(jnp.concatenate(packed, axis=0), spread[...], preferred_element_type=F32)
        hidden = [
            jnp.maximum(pooled[n * channels : (n + 1) * channels] * (1.0 / jnp.maximum(counts[n], 1.0)), 0.0).astype(BF16)
            for n in range(STEP)
        ]
        for half in range(0, STEP, 2):
            for n, row in enumerate(project_rows(final_weights_ref[...], hidden[half : half + 2])):
                at = first + half + n
                out_ref[at] = (trunk_ref[at].astype(F32) + row).astype(BF16)
        return carry

    lax.fori_loop(0, GROUP // STEP, body, 0)


def gather_sides(rows_n, cols_n, unit, q, p, pair_ref, sides):
    units, height, width = pair_ref.shape[1:]
    per_slot = units // p * q // 2
    channel = pl.program_id(0)

    @pl.when(channel == 0)
    def _():
        if height < unit:
            sides[...] = jnp.zeros_like(sides)

    keep = (lanes_of((1, width)) < width // q * p).astype(F32).astype(BF16)
    for side in range(2):
        index = side * per_slot + channel
        first = index // q * p

        def fill(block, side=side):
            def fill_rows(r, carry):
                rows = pl.ds(pl.multiple_of(r * unit, unit), height)
                for c in range(cols_n):
                    sides[side, rows, c * width : (c + 1) * width] = block(r * cols_n + c)
                return carry

            lax.fori_loop(0, rows_n, fill_rows, 0)

        if q == 1:
            fill(lambda slot, index=index: pair_ref[slot, index])
            continue

        @pl.when(lax.rem(index, q) < p)
        def _(fill=fill, index=index, first=first):
            fill(lambda slot: pair_ref[slot, first + lax.rem(index, q)] * keep)

        if (side + 1) * per_slot % q == 0:

            @pl.when(lax.rem(index, q) == p)
            def _(fill=fill, first=first):
                fill(
                    lambda slot: unpack_last(
                        [pair_ref[slot, first + e].astype(F32) for e in range(p)], q, p
                    ).astype(BF16)
                )


def triangle_kernel(contract, rows_n, cols_n, unit, q, p, pair_ref, tri_ref, sides):
    gather_sides(rows_n, cols_n, unit, q, p, pair_ref, sides)
    out = lax.dot_general(
        sides[0], sides[1], (((contract,), (contract,)), ((), ())), preferred_element_type=F32
    )
    height, width = tri_ref.shape[2:]
    for r in range(rows_n):
        for c in range(cols_n):
            tri_ref[r * cols_n + c, 0] = out[
                r * unit : r * unit + height, c * width : (c + 1) * width
            ].astype(BF16)


def triangle(contract, rows_n, cols_n, unit, q, p, pairs, name):
    slots, units, height, width = pairs.shape
    per_slot = units // p * q // 2
    return pl.pallas_call(
        functools.partial(triangle_kernel, contract, rows_n, cols_n, unit, q, p),
        grid=(per_slot,),
        in_specs=[pl.BlockSpec(pairs.shape, lambda c: (0, 0, 0, 0))],
        out_specs=pl.BlockSpec((slots, 1, height, width), lambda c: (0, c, 0, 0)),
        out_shape=jax.ShapeDtypeStruct((slots, per_slot, height, width), BF16),
        scratch_shapes=[pltpu.VMEM((2, rows_n * unit, cols_n * width), BF16)],
        name=name,
    )(pairs)


SMEM = pl.BlockSpec(memory_space=pltpu.SMEM)
ANY = pl.BlockSpec(memory_space=pl.ANY)


def whole_block(array):
    zeros = (0,) * array.ndim
    return pl.BlockSpec(array.shape, lambda g: zeros)


def rows_block(*rest):
    zeros = (0,) * len(rest)
    return pl.BlockSpec((GROUP,) + rest, lambda g: (g,) + zeros)


def with_capacity(
    capacity,
    counts,
    template_pair,
    trunk,
    coverage,
    chain_ids,
    chain_vec,
    trunk_weights,
    proj_weights,
    out_weights,
    final_weights,
):
    unit, trunk_channels, tile_cols = trunk.shape
    channels = template_pair.shape[2]
    rows_n, cols_n = lax.axis_size("row"), lax.axis_size("col")
    slots = rows_n * cols_n
    per_slot = channels // slots
    grid = (pl.cdiv(capacity, GROUP),)
    stacked = proj_weights.reshape(2, 5 * channels, channels)
    chain_all = chain_ids[None]
    chain_column = chain_vec[:, None]

    q, p = packing(capacity, unit, tile_cols, per_slot)
    units = 2 * per_slot // q * p
    pair_spec = pl.BlockSpec((slots, units, GROUP, tile_cols), lambda g: (0, 0, g, 0))
    pair_shape = jax.ShapeDtypeStruct((slots, units, capacity, tile_cols), BF16)
    rep_spec = rows_block(channels, tile_cols)
    rep_shape = jax.ShapeDtypeStruct((capacity, channels, tile_cols), BF16)
    trunk_spec = rows_block(trunk_channels, tile_cols)
    tri_spec = pl.BlockSpec((channels, GROUP, tile_cols), lambda g: (0, g, 0))
    scratch = pltpu.VMEM((2, GROUP * (channels + PAD), tile_cols), F32)
    tri_scratch = pltpu.VMEM((channels * (GROUP + PAD), tile_cols), F32)
    gated_outs = dict(
        out_specs=[pair_spec, rep_spec, rep_spec], out_shape=[pair_shape, rep_shape, rep_shape]
    )

    def exchange(values):
        return lax.all_to_all(values, ("row", "col"), 0, 0, tiled=True)

    pairs, rep, gate = pl.pallas_call(
        functools.partial(pre_kernel, unit, q, p),
        grid=grid,
        in_specs=[
            SMEM,
            SMEM,
            SMEM,
            ANY,
            ANY,
            whole_block(coverage),
            whole_block(chain_all),
            whole_block(chain_column),
            whole_block(trunk_weights),
            whole_block(stacked[0]),
        ],
        scratch_shapes=[
            scratch,
            pltpu.VMEM((2, GROUP, channels, tile_cols), BF16),
            pltpu.VMEM((2, GROUP, trunk_channels, tile_cols), BF16),
            pltpu.SMEM((unit,), jnp.int32),
            pltpu.VMEM((tile_cols, tile_cols), BF16),
            pltpu.SemaphoreType.DMA((2, 2, GROUP)),
        ],
        name="pre",
        **gated_outs,
    )(coverage, chain_ids, counts, template_pair, trunk, coverage, chain_all, chain_column, trunk_weights, stacked[0])

    tri = exchange(triangle(1, rows_n, cols_n, unit, q, p, exchange(pairs), "outgoing"))
    pairs, rep, gate = pl.pallas_call(
        functools.partial(mid_kernel, unit, q, p),
        grid=grid,
        in_specs=[SMEM, tri_spec, rep_spec, rep_spec, whole_block(out_weights[0]), whole_block(stacked[1])],
        scratch_shapes=[scratch, tri_scratch],
        name="mid",
        **gated_outs,
    )(counts, tri.reshape(channels, capacity, tile_cols), rep, gate, out_weights[0], stacked[1])

    tri = exchange(triangle(0, rows_n, cols_n, unit, q, p, exchange(pairs), "incoming"))
    pooled = pl.pallas_call(
        last_kernel,
        grid=grid,
        in_specs=[tri_spec, rep_spec, rep_spec, whole_block(out_weights[1])],
        out_specs=rep_spec,
        out_shape=rep_shape,
        scratch_shapes=[tri_scratch],
        name="last",
    )(tri.reshape(channels, capacity, tile_cols), rep, gate, out_weights[1])

    other = lax.ppermute(pooled, "tmpl", [(0, 1), (1, 0)])
    return pl.pallas_call(
        functools.partial(finish_kernel, unit),
        grid=(unit // GROUP,),
        in_specs=[
            SMEM,
            whole_block(pooled),
            whole_block(pooled),
            trunk_spec,
            whole_block(coverage),
            whole_block(final_weights),
        ],
        out_specs=trunk_spec,
        out_shape=jax.ShapeDtypeStruct(trunk.shape, BF16),
        scratch_shapes=[pltpu.SMEM((2, unit), jnp.int32), pltpu.VMEM((2 * tile_cols, tile_cols), BF16)],
        name="finish",
    )(coverage, pooled, other, trunk, coverage, final_weights)


def per_device(template_pair, trunk, coverage, *rest):
    unit, _, tile_cols = trunk.shape
    templates, tokens = coverage.shape
    counts = jnp.sum(coverage.reshape(templates, tokens // unit, unit), axis=2)
    capacities = [unit]
    if unit == tile_cols and unit % 16 == 0:
        capacities = [unit * share // 16 for share in (12, 13, 14, 16)]
    args = (counts, template_pair, trunk, coverage) + rest
    if len(capacities) == 1:
        return with_capacity(unit, *args)
    most = jnp.max(counts)
    branch = sum((most > capacity).astype(jnp.int32) for capacity in capacities[:-1])
    return lax.switch(branch, [functools.partial(with_capacity, capacity) for capacity in capacities], *args)


def solution(mesh):
    in_specs = (
        P("tmpl", "row", None, "col"),
        P("row", None, "col"),
        P(),
        P(),
        P(),
        P(),
        P(),
        P(),
        P(),
    )
    out_specs = P("row", None, "col")
    return jax.shard_map(
        per_device, mesh=mesh, in_specs=in_specs, out_specs=out_specs, check_vma=False
    )
```

```python
import functools

import jax
import jax.numpy as jnp
from jax import lax
from jax.experimental import pallas as pl
from jax.experimental.pallas import tpu as pltpu
from jax.sharding import PartitionSpec as P

epsilon = 1e-05
GROUP = 16
F32 = jnp.float32
BF16 = jnp.bfloat16


def sigmoid(x):
    return 0.5 * jnp.tanh(0.5 * x) + 0.5


def norm_rows(x):
    scale = 1.0 / x.shape[0]
    centred = x - jnp.sum(x, axis=0, keepdims=True) * scale
    spread = jnp.sum(centred * centred, axis=0, keepdims=True) * scale
    return centred * lax.rsqrt(spread + epsilon)


def project_rows(weights, rows):
    wide = jnp.concatenate(rows, axis=1)
    out = jnp.dot(weights, wide, preferred_element_type=F32)
    cols = rows[0].shape[1]
    return [out[:, n * cols : (n + 1) * cols] for n in range(len(rows))]


def emit_gated(reps, masks, first, weights_ref, gate_ref, scratch):
    channels = reps[0].shape[0]
    normed = [norm_rows(rep).astype(BF16) for rep in reps]
    for half in range(0, len(reps), 2):
        pieces = project_rows(weights_ref[...], normed[half : half + 2])
        for n, piece in enumerate(pieces):
            p = [piece[k * channels : (k + 1) * channels] for k in range(5)]
            at = first + half + n
            rows = pl.ds(pl.multiple_of(at * (channels + PAD), 8), channels)
            mask = masks[half + n]
            scratch[0, rows, :] = mask * sigmoid(p[0]) * p[1]
            scratch[1, rows, :] = mask * sigmoid(p[2]) * p[3]
            gate_ref[at] = sigmoid(p[4]).astype(gate_ref.dtype)


def packing(capacity, unit, width, per_slot):
    if unit == width:
        for q, p in ((4, 3), (8, 7)):
            if capacity * q <= width * p and 2 * per_slot % q == 0:
                return q, p
    return 1, 1


def lanes_of(shape, dtype=jnp.int32):
    return lax.broadcasted_iota(dtype, shape, len(shape) - 1)


def pack(units, q, p):
    if q == 1:
        return units
    width = units[0].shape[-1]
    kept, piece = width // q * p, width // q
    free = lanes_of(units[0].shape) >= kept
    out = []
    for first in range(0, len(units), q):
        last = units[first + q - 1]
        for e in range(p):
            out.append(jnp.where(free, pltpu.roll(last, kept - e * piece, 1), units[first + e]))
    return out


def unpack_last(packed, q, p):
    width = packed[0].shape[-1]
    piece = width // q
    at = lanes_of(packed[0].shape) // piece
    out = jnp.zeros_like(packed[0])
    for e in range(p):
        out = jnp.where(at == e, pltpu.roll(packed[e], (e + 1) * piece, 1), out)
    return out


def store_by_channel(q, p, scratch, pair_ref):
    slots, units = pair_ref.shape[:2]
    per_slot = units // p * q // 2
    channels = slots * per_slot
    for slot in range(slots):
        values = [
            scratch[side, pl.ds(slot * per_slot + channel, GROUP, stride=channels + PAD), :]
            for side in range(2)
            for channel in range(per_slot)
        ]
        for n, value in enumerate(pack(values, q, p)):
            pair_ref[slot, n] = value.astype(BF16)


STEP = 16
PAD = 8


def block_mask(counts_ref, width, unit):
    template = lax.axis_index("tmpl")
    lanes = lax.broadcasted_iota(jnp.int32, (1, width), 1)
    owners = width // unit
    first = lax.axis_index("col") * owners
    mask = jnp.zeros((1, width), F32)
    for owner in range(owners):
        low = owner * unit
        inside = (lanes >= low) & (lanes < low + counts_ref[template, first + owner])
        mask = jnp.where(inside, 1.0, mask)
    return mask


def selection(cover, unit):
    width = cover.shape[1]
    source = lax.broadcasted_iota(jnp.int32, (width, width), 0)
    target = lax.broadcasted_iota(jnp.int32, (width, width), 1)
    upper = ((source <= target) & (source // unit == target // unit)).astype(F32).astype(BF16)
    wide = jnp.broadcast_to(cover, (GROUP, width)).astype(BF16)
    ranks = jnp.dot(wide, upper, preferred_element_type=F32)[:1].astype(jnp.int32)
    slots = target[:1] // unit * unit + ranks - 1
    return jnp.where((source == slots) & (cover > 0.5), 1.0, 0.0)


def template_row(rows, template):
    out = rows[:1]
    for t in range(1, rows.shape[0]):
        out = jnp.where(template == t, rows[t : t + 1], out)
    return out


def pre_kernel(unit, q, p, cover_ref, chain_ref, counts_ref, tp_hbm, trunk_hbm, cover_all_ref, chain_all_ref, chain_vec_ref,
               trunk_weights_ref, weights_ref, pair_ref, rep_ref, gate_ref,
               scratch, tp_buffer, trunk_buffer, order, pick, sems):
    step_id = pl.program_id(0)
    base = step_id * GROUP
    cols = tp_buffer.shape[3]
    channels = tp_buffer.shape[2]
    template = lax.axis_index("tmpl")
    row_start = lax.axis_index("row") * unit
    col_start = pl.multiple_of(lax.axis_index("col") * cols, cols)
    slot = lax.rem(step_id, 2)

    def copies(group, into):
        out = []
        for n in range(GROUP):
            row = order[group * GROUP + n]
            out.append(pltpu.make_async_copy(tp_hbm.at[0, row], tp_buffer.at[into, n], sems.at[into, 0, n]))
            out.append(pltpu.make_async_copy(trunk_hbm.at[row], trunk_buffer.at[into, n], sems.at[into, 1, n]))
        return out

    @pl.when(step_id == 0)
    def _():
        def place(row, taken):
            covered = cover_ref[template, row_start + row]
            order[jnp.where(covered > 0, taken, unit - 1 - (row - taken))] = row
            return taken + covered

        lax.fori_loop(0, unit, place, 0, unroll=8)
        for copy in copies(0, 0):
            copy.start()
        cover = template_row(cover_all_ref[:, pl.ds(col_start, cols)].astype(F32), template)
        pick[...] = jnp.transpose(selection(cover, unit)).astype(BF16)

    @pl.when(step_id + 1 < pl.num_programs(0))
    def _():
        for copy in copies(step_id + 1, 1 - slot):
            copy.start()

    for copy in copies(step_id, slot):
        copy.wait()

    trunk_weights = trunk_weights_ref[...]
    weight_sums = jnp.sum(trunk_weights.astype(F32), axis=1, keepdims=True)
    chain_cols = chain_all_ref[:, pl.ds(col_start, cols)]
    col_mask = block_mask(counts_ref, cols, unit)
    row_count = counts_ref[template, lax.axis_index("row")]

    def body(step, carry):
        first = step * STEP
        raw, masks = [], []
        rows = [trunk_buffer[slot, first + n] for n in range(STEP)]
        projected = []
        for half in range(0, STEP, 2):
            projected += project_rows(trunk_weights, rows[half : half + 2])
        for n in range(STEP):
            at = first + n
            values = rows[n].astype(F32)
            scale = 1.0 / values.shape[0]
            centre = jnp.sum(values, axis=0, keepdims=True) * scale
            centred = values - centre
            spread = jnp.sum(centred * centred, axis=0, keepdims=True) * scale
            trunk_proj = (projected[n] - weight_sums * centre) * lax.rsqrt(spread + epsilon)
            same = (chain_cols == chain_ref[row_start + order[base + at]]).astype(F32)
            raw.append((tp_buffer[slot, at].astype(F32) + same * chain_vec_ref[...] + trunk_proj).astype(BF16))
            masks.append(jnp.where(base + at < row_count, col_mask, 0.0))
        picked = jnp.dot(jnp.concatenate(raw, axis=0), pick[...], preferred_element_type=F32)
        reps = [picked[n * channels : (n + 1) * channels] for n in range(STEP)]
        for n in range(STEP):
            rep_ref[first + n] = reps[n].astype(BF16)
        emit_gated(reps, masks, first, weights_ref, gate_ref, scratch)
        return carry

    lax.fori_loop(0, GROUP // STEP, body, 0)
    store_by_channel(q, p, scratch, pair_ref)


def returned_rows(capacity, per_slot, q):
    if q == 1:
        return per_slot * capacity
    left = per_slot - 1
    return left * capacity + (8 * pl.cdiv(capacity, 16) if left < q - 1 else 0)


def load_tri(capacity, q, tri_ref, tri_scratch):
    slots, _, width = tri_ref.shape
    channels = tri_scratch.shape[0] // (GROUP + PAD)
    per_slot = channels // slots
    scale = 1.0 / channels
    base = pl.program_id(0) * GROUP
    total = jnp.zeros((GROUP, width), F32)
    whole = per_slot if q == 1 else per_slot - 1
    piece = width // q
    lanes = lanes_of((GROUP, width))
    for slot in range(slots):
        units = [
            tri_ref[slot, pl.ds(pl.multiple_of(e * capacity + base, 8), GROUP), :].astype(F32) for e in range(whole)
        ]
        if whole < per_slot:
            last = jnp.zeros_like(total)
            for e in range(whole):
                last = jnp.where(lanes // piece == e, pltpu.roll(units[e], (e + 1) * piece, 1), last)
            if whole < q - 1:
                start = whole * piece
                half = (width - piece - start) % width
                at = pl.multiple_of(whole * capacity + pl.program_id(0) * 8, 8)
                folded = tri_ref[slot, pl.ds(at, 8), :].astype(F32)
                rest = jnp.concatenate(
                    [pltpu.roll(folded, start, 1), pltpu.roll(folded, width + start - half, 1)], axis=0
                )
                last = jnp.where(lanes < start, last, rest)
            units.append(last)
        for e, value in enumerate(units):
            at = (slot * per_slot + e) * (GROUP + PAD)
            tri_scratch[at : at + GROUP, :] = value
            total += value
    centre = total * scale
    total = jnp.zeros_like(total)
    for channel in range(channels):
        at = channel * (GROUP + PAD)
        centred = tri_scratch[at : at + GROUP, :] - centre
        total += centred * centred
    inverse = lax.rsqrt(total * scale + epsilon)
    for channel in range(channels):
        at = channel * (GROUP + PAD)
        tri_scratch[at : at + GROUP, :] = (tri_scratch[at : at + GROUP, :] - centre) * inverse


def updated_rows(first, tri_scratch, rep_ref, gate_ref, out_weights_ref):
    channels = rep_ref.shape[1]
    normed = [
        tri_scratch[pl.ds(first + n, channels, stride=GROUP + PAD), :].astype(BF16) for n in range(STEP)
    ]
    projected = []
    for half in range(0, STEP, 2):
        projected += project_rows(out_weights_ref[...], normed[half : half + 2])
    return [
        (rep_ref[first + n].astype(F32) + gate_ref[first + n].astype(F32) * projected[n]).astype(BF16)
        for n in range(STEP)
    ]


def mid_kernel(unit, capacity, q, p, counts_ref, tri_ref, rep_in_ref, gate_in_ref, out_weights_ref, weights_ref,
               pair_ref, rep_ref, gate_ref, scratch, tri_scratch):
    base = pl.program_id(0) * GROUP
    load_tri(capacity, q, tri_ref, tri_scratch)
    col_mask = block_mask(counts_ref, rep_ref.shape[2], unit)
    row_count = counts_ref[lax.axis_index("tmpl"), lax.axis_index("row")]

    def body(step, carry):
        first = step * STEP
        rows = updated_rows(first, tri_scratch, rep_in_ref, gate_in_ref, out_weights_ref)
        masks = []
        for n in range(STEP):
            rep_ref[first + n] = rows[n]
            masks.append(jnp.where(base + first + n < row_count, col_mask, 0.0))
        emit_gated([row.astype(F32) for row in rows], masks, first, weights_ref, gate_ref, scratch)
        return carry

    lax.fori_loop(0, GROUP // STEP, body, 0)
    store_by_channel(q, p, scratch, pair_ref)


def last_kernel(capacity, q, tri_ref, rep_in_ref, gate_in_ref, out_weights_ref, pooled_ref, tri_scratch):
    load_tri(capacity, q, tri_ref, tri_scratch)

    def body(step, carry):
        first = step * STEP
        rows = updated_rows(first, tri_scratch, rep_in_ref, gate_in_ref, out_weights_ref)
        for n in range(STEP):
            pooled_ref[first + n] = norm_rows(rows[n].astype(F32)).astype(BF16)
        return carry

    lax.fori_loop(0, GROUP // STEP, body, 0)


def finish_kernel(unit, cover_ref, mine_ref, other_ref, trunk_ref, cover_all_ref, final_weights_ref, out_ref,
                  place, spread):
    step_id = pl.program_id(0)
    base = step_id * GROUP
    cols = out_ref.shape[2]
    channels = mine_ref.shape[1]
    template = lax.axis_index("tmpl")
    templates = (template, 1 - template)
    row_start = lax.axis_index("row") * unit
    col_start = pl.multiple_of(lax.axis_index("col") * cols, cols)
    cover_cols = cover_all_ref[:, pl.ds(col_start, cols)].astype(F32)
    covers = [template_row(cover_cols, t) for t in templates]

    @pl.when(step_id == 0)
    def _():
        def count(row, taken):
            out = []
            for k, t in enumerate(templates):
                covered = cover_ref[t, row_start + row]
                place[k, row] = jnp.where(covered > 0, taken[k], 0)
                out.append(taken[k] + covered)
            return tuple(out)

        lax.fori_loop(0, unit, count, (0,) * len(templates), unroll=8)
        for k in range(len(templates)):
            spread[k * cols : (k + 1) * cols, :] = selection(covers[k], unit).astype(BF16)

    def body(step, carry):
        first = step * STEP
        packed, counts = [], []
        for n in range(STEP):
            row = base + first + n
            parts = []
            count = jnp.zeros_like(covers[0])
            for k, (t, ref) in enumerate(zip(templates, (mine_ref, other_ref))):
                covered = cover_ref[t, row_start + row]
                value = ref[place[k, row]].astype(F32)
                parts.append(jnp.where(covered > 0, value, 0.0).astype(BF16))
                count += covers[k] * covered.astype(F32)
            packed.append(jnp.concatenate(parts, axis=1))
            counts.append(count)
        pooled = jnp.dot(jnp.concatenate(packed, axis=0), spread[...], preferred_element_type=F32)
        hidden = [
            jnp.maximum(pooled[n * channels : (n + 1) * channels] * (1.0 / jnp.maximum(counts[n], 1.0)), 0.0).astype(BF16)
            for n in range(STEP)
        ]
        for half in range(0, STEP, 2):
            for n, row in enumerate(project_rows(final_weights_ref[...], hidden[half : half + 2])):
                at = first + half + n
                out_ref[at] = (trunk_ref[at].astype(F32) + row).astype(BF16)
        return carry

    lax.fori_loop(0, GROUP // STEP, body, 0)


def gather_sides(rows_n, cols_n, unit, q, p, pair_ref, sides):
    units, height, width = pair_ref.shape[1:]
    per_slot = units // p * q // 2
    channel = per_slot - 1 - pl.program_id(0)

    @pl.when(pl.program_id(0) == 0)
    def _():
        if height < unit:
            sides[...] = jnp.zeros_like(sides)

    keep = (lanes_of((1, width)) < width // q * p).astype(F32).astype(BF16)
    for side in range(2):
        index = side * per_slot + channel
        first = index // q * p

        def fill(block, side=side):
            def fill_rows(r, carry):
                rows = pl.ds(pl.multiple_of(r * unit, unit), height)
                for c in range(cols_n):
                    sides[side, rows, c * width : (c + 1) * width] = block(r * cols_n + c)
                return carry

            lax.fori_loop(0, rows_n, fill_rows, 0)

        if q == 1:
            fill(lambda slot, index=index: pair_ref[slot, index])
            continue

        @pl.when(lax.rem(index, q) < p)
        def _(fill=fill, index=index, first=first):
            fill(lambda slot: pair_ref[slot, first + lax.rem(index, q)] * keep)

        if (side + 1) * per_slot % q == 0:

            @pl.when(lax.rem(index, q) == p)
            def _(fill=fill, first=first):
                fill(
                    lambda slot: unpack_last(
                        [pair_ref[slot, first + e].astype(F32) for e in range(p)], q, p
                    ).astype(BF16)
                )


def triangle_kernel(contract, rows_n, cols_n, unit, q, p, pair_ref, tri_ref, sides, cut):
    gather_sides(rows_n, cols_n, unit, q, p, pair_ref, sides)
    out = lax.dot_general(
        sides[0], sides[1], (((contract,), (contract,)), ((), ())), preferred_element_type=F32
    )
    capacity, width = pair_ref.shape[2:]
    per_slot = pair_ref.shape[1] // p * q // 2
    channel = per_slot - 1 - pl.program_id(0)
    blocks = [
        (r * cols_n + c, out[r * unit : (r + 1) * unit, c * width : (c + 1) * width])
        for r in range(rows_n)
        for c in range(cols_n)
    ]
    place = pl.ds(pl.multiple_of(channel * capacity, 8), capacity)
    if q == 1:
        for slot, block in blocks:
            tri_ref[slot, place, :] = block[:capacity].astype(BF16)
        return

    piece = width // q
    kept = width - piece

    @pl.when(channel == per_slot - 1)
    def _():
        whole = per_slot - 1
        start = whole * piece
        folds = tri_ref.shape[1] - whole * capacity
        for slot, block in blocks:
            cut[slot] = block[:capacity]
            if folds:
                half = kept - start
                tiles = block[: 2 * folds].reshape(folds // 8, 2, 8, width)
                first = tiles[:, 0].reshape(folds, width)
                second = tiles[:, 1].reshape(folds, width)
                folded = jnp.where(
                    lanes_of(first.shape) < half,
                    pltpu.roll(first, width - start, 1),
                    pltpu.roll(second, (half - start) % width, 1),
                )
                tri_ref[slot, whole * capacity :, :] = folded.astype(BF16)

    @pl.when(channel < per_slot - 1)
    def _():
        for slot, block in blocks:
            free = lanes_of((capacity, width)) >= kept
            moved = pltpu.roll(cut[slot], kept - channel * piece, 1)
            tri_ref[slot, place, :] = jnp.where(free, moved, block[:capacity]).astype(BF16)


def triangle(contract, rows_n, cols_n, unit, q, p, pairs, name):
    slots, units, capacity, width = pairs.shape
    per_slot = units // p * q // 2
    shape = (slots, returned_rows(capacity, per_slot, q), width)
    cut = (slots, capacity, width) if q > 1 else (1, 8, width)
    return pl.pallas_call(
        functools.partial(triangle_kernel, contract, rows_n, cols_n, unit, q, p),
        grid=(per_slot,),
        in_specs=[pl.BlockSpec(pairs.shape, lambda c: (0, 0, 0, 0))],
        out_specs=pl.BlockSpec(shape, lambda c: (0, 0, 0)),
        out_shape=jax.ShapeDtypeStruct(shape, BF16),
        scratch_shapes=[pltpu.VMEM((2, rows_n * unit, cols_n * width), BF16), pltpu.VMEM(cut, F32)],
        name=name,
    )(pairs)


SMEM = pl.BlockSpec(memory_space=pltpu.SMEM)
ANY = pl.BlockSpec(memory_space=pl.ANY)


def whole_block(array):
    zeros = (0,) * array.ndim
    return pl.BlockSpec(array.shape, lambda g: zeros)


def rows_block(*rest):
    zeros = (0,) * len(rest)
    return pl.BlockSpec((GROUP,) + rest, lambda g: (g,) + zeros)


def with_capacity(
    capacity,
    counts,
    template_pair,
    trunk,
    coverage,
    chain_ids,
    chain_vec,
    trunk_weights,
    proj_weights,
    out_weights,
    final_weights,
):
    unit, trunk_channels, tile_cols = trunk.shape
    channels = template_pair.shape[2]
    rows_n, cols_n = lax.axis_size("row"), lax.axis_size("col")
    slots = rows_n * cols_n
    per_slot = channels // slots
    grid = (pl.cdiv(capacity, GROUP),)
    q, p = packing(capacity, unit, tile_cols, per_slot)
    stacked = proj_weights.reshape(2, 5 * channels, channels)
    chain_all = chain_ids[None]
    chain_column = chain_vec[:, None]

    units = 2 * per_slot // q * p
    pair_spec = pl.BlockSpec((slots, units, GROUP, tile_cols), lambda g: (0, 0, g, 0))
    pair_shape = jax.ShapeDtypeStruct((slots, units, capacity, tile_cols), BF16)
    rep_spec = rows_block(channels, tile_cols)
    rep_shape = jax.ShapeDtypeStruct((capacity, channels, tile_cols), BF16)
    trunk_spec = rows_block(trunk_channels, tile_cols)
    tri_spec = pl.BlockSpec((slots, returned_rows(capacity, per_slot, q), tile_cols), lambda g: (0, 0, 0))
    scratch = pltpu.VMEM((2, GROUP * (channels + PAD), tile_cols), F32)
    tri_scratch = pltpu.VMEM((channels * (GROUP + PAD), tile_cols), F32)
    gated_outs = dict(
        out_specs=[pair_spec, rep_spec, rep_spec], out_shape=[pair_shape, rep_shape, rep_shape]
    )

    def exchange(values):
        return lax.all_to_all(values, ("row", "col"), 0, 0, tiled=True)

    pairs, rep, gate = pl.pallas_call(
        functools.partial(pre_kernel, unit, q, p),
        grid=grid,
        in_specs=[
            SMEM,
            SMEM,
            SMEM,
            ANY,
            ANY,
            whole_block(coverage),
            whole_block(chain_all),
            whole_block(chain_column),
            whole_block(trunk_weights),
            whole_block(stacked[0]),
        ],
        scratch_shapes=[
            scratch,
            pltpu.VMEM((2, GROUP, channels, tile_cols), BF16),
            pltpu.VMEM((2, GROUP, trunk_channels, tile_cols), BF16),
            pltpu.SMEM((unit,), jnp.int32),
            pltpu.VMEM((tile_cols, tile_cols), BF16),
            pltpu.SemaphoreType.DMA((2, 2, GROUP)),
        ],
        name="pre",
        **gated_outs,
    )(coverage, chain_ids, counts, template_pair, trunk, coverage, chain_all, chain_column, trunk_weights, stacked[0])

    tri = exchange(triangle(1, rows_n, cols_n, unit, q, p, exchange(pairs), "outgoing"))
    pairs, rep, gate = pl.pallas_call(
        functools.partial(mid_kernel, unit, capacity, q, p),
        grid=grid,
        in_specs=[SMEM, tri_spec, rep_spec, rep_spec, whole_block(out_weights[0]), whole_block(stacked[1])],
        scratch_shapes=[scratch, tri_scratch],
        name="mid",
        **gated_outs,
    )(counts, tri, rep, gate, out_weights[0], stacked[1])

    tri = exchange(triangle(0, rows_n, cols_n, unit, q, p, exchange(pairs), "incoming"))
    pooled = pl.pallas_call(
        functools.partial(last_kernel, capacity, q),
        grid=grid,
        in_specs=[tri_spec, rep_spec, rep_spec, whole_block(out_weights[1])],
        out_specs=rep_spec,
        out_shape=rep_shape,
        scratch_shapes=[tri_scratch],
        name="last",
    )(tri, rep, gate, out_weights[1])

    other = lax.ppermute(pooled, "tmpl", [(0, 1), (1, 0)])
    return pl.pallas_call(
        functools.partial(finish_kernel, unit),
        grid=(unit // GROUP,),
        in_specs=[
            SMEM,
            whole_block(pooled),
            whole_block(pooled),
            trunk_spec,
            whole_block(coverage),
            whole_block(final_weights),
        ],
        out_specs=trunk_spec,
        out_shape=jax.ShapeDtypeStruct(trunk.shape, BF16),
        scratch_shapes=[pltpu.SMEM((2, unit), jnp.int32), pltpu.VMEM((2 * tile_cols, tile_cols), BF16)],
        name="finish",
    )(coverage, pooled, other, trunk, coverage, final_weights)


def per_device(template_pair, trunk, coverage, *rest):
    unit, _, tile_cols = trunk.shape
    templates, tokens = coverage.shape
    counts = jnp.sum(coverage.reshape(templates, tokens // unit, unit), axis=2)
    capacities = [unit]
    if unit == tile_cols and unit % 16 == 0:
        capacities = [unit * share // 16 for share in (12, 13, 14, 16)]
    args = (counts, template_pair, trunk, coverage) + rest
    if len(capacities) == 1:
        return with_capacity(unit, *args)
    most = jnp.max(counts)
    branch = sum((most > capacity).astype(jnp.int32) for capacity in capacities[:-1])
    return lax.switch(branch, [functools.partial(with_capacity, capacity) for capacity in capacities], *args)


def solution(mesh):
    in_specs = (
        P("tmpl", "row", None, "col"),
        P("row", None, "col"),
        P(),
        P(),
        P(),
        P(),
        P(),
        P(),
        P(),
    )
    out_specs = P("row", None, "col")
    return jax.shard_map(
        per_device, mesh=mesh, in_specs=in_specs, out_specs=out_specs, check_vma=False
    )
```

```python
import functools

import jax
import jax.numpy as jnp
from jax import lax
from jax.experimental import pallas as pl
from jax.experimental.pallas import tpu as pltpu
from jax.sharding import PartitionSpec as P

epsilon = 1e-05
GROUP = 16
F32 = jnp.float32
BF16 = jnp.bfloat16


def sigmoid(x):
    return 0.5 * jnp.tanh(0.5 * x) + 0.5


def norm_rows(x):
    scale = 1.0 / x.shape[0]
    centred = x - jnp.sum(x, axis=0, keepdims=True) * scale
    spread = jnp.sum(centred * centred, axis=0, keepdims=True) * scale
    return centred * lax.rsqrt(spread + epsilon)


def project_rows(weights, rows):
    wide = jnp.concatenate(rows, axis=1)
    out = jnp.dot(weights, wide, preferred_element_type=F32)
    cols = rows[0].shape[1]
    return [out[:, n * cols : (n + 1) * cols] for n in range(len(rows))]


def emit_gated(reps, masks, first, weights_ref, gate_ref, scratch):
    channels = reps[0].shape[0]
    weights = weights_ref[0].reshape(5 * channels, channels)
    normed = [norm_rows(rep).astype(BF16) for rep in reps]
    for half in range(0, len(reps), 2):
        pieces = project_rows(weights, normed[half : half + 2])
        for n, piece in enumerate(pieces):
            p = [piece[k * channels : (k + 1) * channels] for k in range(5)]
            at = first + half + n
            rows = pl.ds(pl.multiple_of(at * (channels + PAD), 8), channels)
            mask = masks[half + n]
            scratch[0, rows, :] = mask * sigmoid(p[0]) * p[1]
            scratch[1, rows, :] = mask * sigmoid(p[2]) * p[3]
            gate_ref[at] = sigmoid(p[4]).astype(gate_ref.dtype)


def packing(capacity, unit, width, per_slot):
    if unit == width:
        for q, p in ((4, 3), (8, 7)):
            if capacity * q <= width * p and 2 * per_slot % q == 0:
                return q, p
    return 1, 1


def lanes_of(shape, dtype=jnp.int32):
    return lax.broadcasted_iota(dtype, shape, len(shape) - 1)


def pack(units, q, p):
    if q == 1:
        return units
    width = units[0].shape[-1]
    kept, piece = width // q * p, width // q
    free = lanes_of(units[0].shape) >= kept
    out = []
    for first in range(0, len(units), q):
        last = units[first + q - 1]
        for e in range(p):
            out.append(jnp.where(free, pltpu.roll(last, kept - e * piece, 1), units[first + e]))
    return out


def unpack_last(packed, q, p):
    width = packed[0].shape[-1]
    piece = width // q
    at = lanes_of(packed[0].shape) // piece
    out = jnp.zeros_like(packed[0])
    for e in range(p):
        out = jnp.where(at == e, pltpu.roll(packed[e], (e + 1) * piece, 1), out)
    return out


def store_by_channel(q, p, scratch, pair_ref):
    slots, units = pair_ref.shape[:2]
    per_slot = units // p * q // 2
    channels = slots * per_slot
    for slot in range(slots):
        values = [
            scratch[side, pl.ds(slot * per_slot + channel, GROUP, stride=channels + PAD), :]
            for side in range(2)
            for channel in range(per_slot)
        ]
        for n, value in enumerate(pack(values, q, p)):
            pair_ref[slot, n] = value.astype(BF16)


STEP = 16
PAD = 8


def block_mask(counts_ref, width, unit):
    template = lax.axis_index("tmpl")
    lanes = lax.broadcasted_iota(jnp.int32, (1, width), 1)
    owners = width // unit
    first = lax.axis_index("col") * owners
    mask = jnp.zeros((1, width), F32)
    for owner in range(owners):
        low = owner * unit
        inside = (lanes >= low) & (lanes < low + counts_ref[template, first + owner])
        mask = jnp.where(inside, 1.0, mask)
    return mask


def selection(cover, unit):
    width = cover.shape[1]
    source = lax.broadcasted_iota(jnp.int32, (width, width), 0)
    target = lax.broadcasted_iota(jnp.int32, (width, width), 1)
    upper = ((source <= target) & (source // unit == target // unit)).astype(F32).astype(BF16)
    wide = jnp.broadcast_to(cover, (GROUP, width)).astype(BF16)
    ranks = jnp.dot(wide, upper, preferred_element_type=F32)[:1].astype(jnp.int32)
    slots = target[:1] // unit * unit + ranks - 1
    return jnp.where((source == slots) & (cover > 0.5), 1.0, 0.0)


def template_row(rows, template):
    out = rows[:1]
    for t in range(1, rows.shape[0]):
        out = jnp.where(template == t, rows[t : t + 1], out)
    return out


def pre_kernel(unit, q, p, cover_ref, chain_ref, counts_ref, tp_hbm, trunk_hbm, cover_all_ref, chain_all_ref, chain_vec_ref,
               trunk_weights_ref, weights_ref, pair_ref, rep_ref, gate_ref,
               scratch, tp_buffer, trunk_buffer, order, pick, sems):
    step_id = pl.program_id(0)
    base = step_id * GROUP
    cols = tp_buffer.shape[3]
    channels = tp_buffer.shape[2]
    template = lax.axis_index("tmpl")
    row_start = lax.axis_index("row") * unit
    col_start = pl.multiple_of(lax.axis_index("col") * cols, cols)
    slot = lax.rem(step_id, 2)

    def copies(group, into):
        out = []
        for n in range(GROUP):
            row = order[group * GROUP + n]
            out.append(pltpu.make_async_copy(tp_hbm.at[0, row], tp_buffer.at[into, n], sems.at[into, 0, n]))
            out.append(pltpu.make_async_copy(trunk_hbm.at[row], trunk_buffer.at[into, n], sems.at[into, 1, n]))
        return out

    @pl.when(step_id == 0)
    def _():
        def place(row, taken):
            covered = cover_ref[template, row_start + row]
            order[jnp.where(covered > 0, taken, unit - 1 - (row - taken))] = row
            return taken + covered

        lax.fori_loop(0, unit, place, 0, unroll=8)
        for copy in copies(0, 0):
            copy.start()
        cover = template_row(cover_all_ref[:, pl.ds(col_start, cols)].astype(F32), template)
        pick[...] = jnp.transpose(selection(cover, unit)).astype(BF16)

    @pl.when(step_id + 1 < pl.num_programs(0))
    def _():
        for copy in copies(step_id + 1, 1 - slot):
            copy.start()

    for copy in copies(step_id, slot):
        copy.wait()

    trunk_weights = trunk_weights_ref[...]
    weight_sums = jnp.sum(trunk_weights.astype(F32), axis=1, keepdims=True)
    diagonal = lax.broadcasted_iota(jnp.int32, (channels, channels), 0) == lanes_of((channels, channels))
    chain_column = jnp.sum(jnp.where(diagonal, chain_vec_ref[...], 0.0), axis=1, keepdims=True)
    chain_cols = chain_all_ref[:, pl.ds(col_start, cols)]
    col_mask = block_mask(counts_ref, cols, unit)
    row_count = counts_ref[template, lax.axis_index("row")]

    def body(step, carry):
        first = step * STEP
        raw, masks = [], []
        rows = [trunk_buffer[slot, first + n] for n in range(STEP)]
        projected = []
        for half in range(0, STEP, 2):
            projected += project_rows(trunk_weights, rows[half : half + 2])
        for n in range(STEP):
            at = first + n
            values = rows[n].astype(F32)
            scale = 1.0 / values.shape[0]
            centre = jnp.sum(values, axis=0, keepdims=True) * scale
            centred = values - centre
            spread = jnp.sum(centred * centred, axis=0, keepdims=True) * scale
            trunk_proj = (projected[n] - weight_sums * centre) * lax.rsqrt(spread + epsilon)
            same = (chain_cols == chain_ref[row_start + order[base + at]]).astype(F32)
            raw.append((tp_buffer[slot, at].astype(F32) + same * chain_column + trunk_proj).astype(BF16))
            masks.append(jnp.where(base + at < row_count, col_mask, 0.0))
        picked = jnp.dot(jnp.concatenate(raw, axis=0), pick[...], preferred_element_type=F32)
        reps = [picked[n * channels : (n + 1) * channels] for n in range(STEP)]
        for n in range(STEP):
            rep_ref[first + n] = reps[n].astype(BF16)
        emit_gated(reps, masks, first, weights_ref, gate_ref, scratch)
        return carry

    lax.fori_loop(0, GROUP // STEP, body, 0)
    store_by_channel(q, p, scratch, pair_ref)


def returned_rows(capacity, per_slot, q):
    if q == 1:
        return per_slot * capacity
    left = per_slot - 1
    return left * capacity + (8 * pl.cdiv(capacity, 16) if left < q - 1 else 0)


def load_tri(capacity, q, tri_ref, tri_scratch):
    slots, _, width = tri_ref.shape
    channels = tri_scratch.shape[0] // (GROUP + PAD)
    per_slot = channels // slots
    scale = 1.0 / channels
    base = pl.program_id(0) * GROUP
    total = jnp.zeros((GROUP, width), F32)
    whole = per_slot if q == 1 else per_slot - 1
    piece = width // q
    lanes = lanes_of((GROUP, width))
    for slot in range(slots):
        units = [
            tri_ref[slot, pl.ds(pl.multiple_of(e * capacity + base, 8), GROUP), :].astype(F32) for e in range(whole)
        ]
        if whole < per_slot:
            last = jnp.zeros_like(total)
            for e in range(whole):
                last = jnp.where(lanes // piece == e, pltpu.roll(units[e], (e + 1) * piece, 1), last)
            if whole < q - 1:
                start = whole * piece
                half = (width - piece - start) % width
                at = pl.multiple_of(whole * capacity + pl.program_id(0) * 8, 8)
                folded = tri_ref[slot, pl.ds(at, 8), :].astype(F32)
                rest = jnp.concatenate(
                    [pltpu.roll(folded, start, 1), pltpu.roll(folded, width + start - half, 1)], axis=0
                )
                last = jnp.where(lanes < start, last, rest)
            units.append(last)
        for e, value in enumerate(units):
            at = (slot * per_slot + e) * (GROUP + PAD)
            tri_scratch[at : at + GROUP, :] = value
            total += value
    centre = total * scale
    total = jnp.zeros_like(total)
    for channel in range(channels):
        at = channel * (GROUP + PAD)
        centred = tri_scratch[at : at + GROUP, :] - centre
        total += centred * centred
    inverse = lax.rsqrt(total * scale + epsilon)
    for channel in range(channels):
        at = channel * (GROUP + PAD)
        tri_scratch[at : at + GROUP, :] = (tri_scratch[at : at + GROUP, :] - centre) * inverse


def updated_rows(first, tri_scratch, rep_ref, gate_ref, out_weights_ref):
    channels = rep_ref.shape[1]
    normed = [
        tri_scratch[pl.ds(first + n, channels, stride=GROUP + PAD), :].astype(BF16) for n in range(STEP)
    ]
    projected = []
    for half in range(0, STEP, 2):
        projected += project_rows(out_weights_ref[0], normed[half : half + 2])
    return [
        (rep_ref[first + n].astype(F32) + gate_ref[first + n].astype(F32) * projected[n]).astype(BF16)
        for n in range(STEP)
    ]


def mid_kernel(unit, capacity, q, p, counts_ref, tri_ref, rep_in_ref, gate_in_ref, out_weights_ref, weights_ref,
               pair_ref, rep_ref, gate_ref, scratch, tri_scratch):
    base = pl.program_id(0) * GROUP
    load_tri(capacity, q, tri_ref, tri_scratch)
    col_mask = block_mask(counts_ref, rep_ref.shape[2], unit)
    row_count = counts_ref[lax.axis_index("tmpl"), lax.axis_index("row")]

    def body(step, carry):
        first = step * STEP
        rows = updated_rows(first, tri_scratch, rep_in_ref, gate_in_ref, out_weights_ref)
        masks = []
        for n in range(STEP):
            rep_ref[first + n] = rows[n]
            masks.append(jnp.where(base + first + n < row_count, col_mask, 0.0))
        emit_gated([row.astype(F32) for row in rows], masks, first, weights_ref, gate_ref, scratch)
        return carry

    lax.fori_loop(0, GROUP // STEP, body, 0)
    store_by_channel(q, p, scratch, pair_ref)


def last_kernel(capacity, q, tri_ref, rep_in_ref, gate_in_ref, out_weights_ref, pooled_ref, tri_scratch):
    load_tri(capacity, q, tri_ref, tri_scratch)

    def body(step, carry):
        first = step * STEP
        rows = updated_rows(first, tri_scratch, rep_in_ref, gate_in_ref, out_weights_ref)
        for n in range(STEP):
            pooled_ref[first + n] = norm_rows(rows[n].astype(F32)).astype(BF16)
        return carry

    lax.fori_loop(0, GROUP // STEP, body, 0)


def finish_kernel(unit, cover_ref, mine_ref, other_ref, trunk_ref, cover_all_ref, final_weights_ref, out_ref,
                  place, spread):
    step_id = pl.program_id(0)
    base = step_id * GROUP
    cols = out_ref.shape[2]
    channels = mine_ref.shape[1]
    template = lax.axis_index("tmpl")
    templates = (template, 1 - template)
    row_start = lax.axis_index("row") * unit
    col_start = pl.multiple_of(lax.axis_index("col") * cols, cols)
    cover_cols = cover_all_ref[:, pl.ds(col_start, cols)].astype(F32)
    covers = [template_row(cover_cols, t) for t in templates]

    @pl.when(step_id == 0)
    def _():
        def count(row, taken):
            out = []
            for k, t in enumerate(templates):
                covered = cover_ref[t, row_start + row]
                place[k, row] = jnp.where(covered > 0, taken[k], 0)
                out.append(taken[k] + covered)
            return tuple(out)

        lax.fori_loop(0, unit, count, (0,) * len(templates), unroll=8)
        for k in range(len(templates)):
            spread[k * cols : (k + 1) * cols, :] = selection(covers[k], unit).astype(BF16)

    def body(step, carry):
        first = step * STEP
        packed, counts = [], []
        for n in range(STEP):
            row = base + first + n
            parts = []
            count = jnp.zeros_like(covers[0])
            for k, (t, ref) in enumerate(zip(templates, (mine_ref, other_ref))):
                covered = cover_ref[t, row_start + row]
                value = ref[place[k, row]]
                parts.append(lax.select(covered > 0, value, jnp.zeros_like(value)))
                count += covers[k] * covered.astype(F32)
            packed.append(jnp.concatenate(parts, axis=1))
            counts.append(count)
        pooled = jnp.dot(jnp.concatenate(packed, axis=0), spread[...], preferred_element_type=F32)
        hidden = [
            jnp.maximum(pooled[n * channels : (n + 1) * channels] * (1.0 / jnp.maximum(counts[n], 1.0)), 0.0).astype(BF16)
            for n in range(STEP)
        ]
        for half in range(0, STEP, 2):
            for n, row in enumerate(project_rows(final_weights_ref[...], hidden[half : half + 2])):
                at = first + half + n
                out_ref[at] = (trunk_ref[at].astype(F32) + row).astype(BF16)
        return carry

    lax.fori_loop(0, GROUP // STEP, body, 0)


def gather_sides(rows_n, cols_n, unit, q, p, pair_ref, sides):
    units, height, width = pair_ref.shape[1:]
    per_slot = units // p * q // 2
    channel = per_slot - 1 - pl.program_id(0)

    @pl.when(pl.program_id(0) == 0)
    def _():
        if height < unit:
            sides[...] = jnp.zeros_like(sides)

    keep = (lanes_of((1, width)) < width // q * p).astype(F32).astype(BF16)
    for side in range(2):
        index = side * per_slot + channel
        first = index // q * p

        def fill(block, side=side):
            def fill_rows(r, carry):
                rows = pl.ds(pl.multiple_of(r * unit, unit), height)
                for c in range(cols_n):
                    sides[side, rows, c * width : (c + 1) * width] = block(r * cols_n + c)
                return carry

            lax.fori_loop(0, rows_n, fill_rows, 0)

        if q == 1:
            fill(lambda slot, index=index: pair_ref[slot, index])
            continue

        @pl.when(lax.rem(index, q) < p)
        def _(fill=fill, index=index, first=first):
            fill(lambda slot: pair_ref[slot, first + lax.rem(index, q)] * keep)

        if (side + 1) * per_slot % q == 0:

            @pl.when(lax.rem(index, q) == p)
            def _(fill=fill, first=first):
                fill(
                    lambda slot: unpack_last(
                        [pair_ref[slot, first + e].astype(F32) for e in range(p)], q, p
                    ).astype(BF16)
                )


def triangle_kernel(contract, rows_n, cols_n, unit, q, p, pair_ref, tri_ref, sides, cut):
    gather_sides(rows_n, cols_n, unit, q, p, pair_ref, sides)
    out = lax.dot_general(
        sides[0], sides[1], (((contract,), (contract,)), ((), ())), preferred_element_type=F32
    )
    capacity, width = pair_ref.shape[2:]
    per_slot = pair_ref.shape[1] // p * q // 2
    channel = per_slot - 1 - pl.program_id(0)
    blocks = [
        (r * cols_n + c, out[r * unit : (r + 1) * unit, c * width : (c + 1) * width])
        for r in range(rows_n)
        for c in range(cols_n)
    ]
    place = pl.ds(pl.multiple_of(channel * capacity, 8), capacity)
    if q == 1:
        for slot, block in blocks:
            tri_ref[slot, place, :] = block[:capacity].astype(BF16)
        return

    piece = width // q
    kept = width - piece

    @pl.when(channel == per_slot - 1)
    def _():
        whole = per_slot - 1
        start = whole * piece
        folds = tri_ref.shape[1] - whole * capacity
        for slot, block in blocks:
            cut[slot] = block[:capacity]
            if folds:
                half = kept - start
                tiles = block[: 2 * folds].reshape(folds // 8, 2, 8, width)
                first = tiles[:, 0].reshape(folds, width)
                second = tiles[:, 1].reshape(folds, width)
                folded = jnp.where(
                    lanes_of(first.shape) < half,
                    pltpu.roll(first, width - start, 1),
                    pltpu.roll(second, (half - start) % width, 1),
                )
                tri_ref[slot, whole * capacity :, :] = folded.astype(BF16)

    @pl.when(channel < per_slot - 1)
    def _():
        for slot, block in blocks:
            free = lanes_of((capacity, width)) >= kept
            moved = pltpu.roll(cut[slot], kept - channel * piece, 1)
            tri_ref[slot, place, :] = jnp.where(free, moved, block[:capacity]).astype(BF16)


def triangle(contract, rows_n, cols_n, unit, q, p, pairs, name):
    slots, units, capacity, width = pairs.shape
    per_slot = units // p * q // 2
    shape = (slots, returned_rows(capacity, per_slot, q), width)
    cut = (slots, capacity, width) if q > 1 else (1, 8, width)
    return pl.pallas_call(
        functools.partial(triangle_kernel, contract, rows_n, cols_n, unit, q, p),
        grid=(per_slot,),
        in_specs=[pl.BlockSpec(pairs.shape, lambda c: (0, 0, 0, 0))],
        out_specs=pl.BlockSpec(shape, lambda c: (0, 0, 0)),
        out_shape=jax.ShapeDtypeStruct(shape, BF16),
        scratch_shapes=[pltpu.VMEM((2, rows_n * unit, cols_n * width), BF16), pltpu.VMEM(cut, F32)],
        name=name,
    )(pairs)


SMEM = pl.BlockSpec(memory_space=pltpu.SMEM)
ANY = pl.BlockSpec(memory_space=pl.ANY)


def whole_block(array):
    zeros = (0,) * array.ndim
    return pl.BlockSpec(array.shape, lambda g: zeros)


def update_block(array, number):
    index = (number,) + (0,) * (array.ndim - 1)
    return pl.BlockSpec((1,) + array.shape[1:], lambda g: index)


def rows_block(*rest):
    zeros = (0,) * len(rest)
    return pl.BlockSpec((GROUP,) + rest, lambda g: (g,) + zeros)


def with_capacity(
    capacity,
    counts,
    template_pair,
    trunk,
    coverage,
    chain_ids,
    chain_vec,
    trunk_weights,
    proj_weights,
    out_weights,
    final_weights,
):
    unit, trunk_channels, tile_cols = trunk.shape
    channels = template_pair.shape[2]
    rows_n, cols_n = lax.axis_size("row"), lax.axis_size("col")
    slots = rows_n * cols_n
    per_slot = channels // slots
    grid = (pl.cdiv(capacity, GROUP),)
    q, p = packing(capacity, unit, tile_cols, per_slot)
    chain_all = chain_ids[None]
    chain_row = chain_vec[None]

    units = 2 * per_slot // q * p
    pair_spec = pl.BlockSpec((slots, units, GROUP, tile_cols), lambda g: (0, 0, g, 0))
    pair_shape = jax.ShapeDtypeStruct((slots, units, capacity, tile_cols), BF16)
    rep_spec = rows_block(channels, tile_cols)
    rep_shape = jax.ShapeDtypeStruct((capacity, channels, tile_cols), BF16)
    trunk_spec = rows_block(trunk_channels, tile_cols)
    tri_spec = pl.BlockSpec((slots, returned_rows(capacity, per_slot, q), tile_cols), lambda g: (0, 0, 0))
    scratch = pltpu.VMEM((2, GROUP * (channels + PAD), tile_cols), F32)
    tri_scratch = pltpu.VMEM((channels * (GROUP + PAD), tile_cols), F32)
    gated_outs = dict(
        out_specs=[pair_spec, rep_spec, rep_spec], out_shape=[pair_shape, rep_shape, rep_shape]
    )

    def exchange(values):
        return lax.all_to_all(values, ("row", "col"), 0, 0, tiled=True)

    pairs, rep, gate = pl.pallas_call(
        functools.partial(pre_kernel, unit, q, p),
        grid=grid,
        in_specs=[
            SMEM,
            SMEM,
            SMEM,
            ANY,
            ANY,
            whole_block(coverage),
            whole_block(chain_all),
            whole_block(chain_row),
            whole_block(trunk_weights),
            update_block(proj_weights, 0),
        ],
        scratch_shapes=[
            scratch,
            pltpu.VMEM((2, GROUP, channels, tile_cols), BF16),
            pltpu.VMEM((2, GROUP, trunk_channels, tile_cols), BF16),
            pltpu.SMEM((unit,), jnp.int32),
            pltpu.VMEM((tile_cols, tile_cols), BF16),
            pltpu.SemaphoreType.DMA((2, 2, GROUP)),
        ],
        name="pre",
        **gated_outs,
    )(coverage, chain_ids, counts, template_pair, trunk, coverage, chain_all, chain_row, trunk_weights, proj_weights)

    tri = exchange(triangle(1, rows_n, cols_n, unit, q, p, exchange(pairs), "outgoing"))
    pairs, rep, gate = pl.pallas_call(
        functools.partial(mid_kernel, unit, capacity, q, p),
        grid=grid,
        in_specs=[SMEM, tri_spec, rep_spec, rep_spec, update_block(out_weights, 0), update_block(proj_weights, 1)],
        scratch_shapes=[scratch, tri_scratch],
        name="mid",
        **gated_outs,
    )(counts, tri, rep, gate, out_weights, proj_weights)

    tri = exchange(triangle(0, rows_n, cols_n, unit, q, p, exchange(pairs), "incoming"))
    pooled = pl.pallas_call(
        functools.partial(last_kernel, capacity, q),
        grid=grid,
        in_specs=[tri_spec, rep_spec, rep_spec, update_block(out_weights, 1)],
        out_specs=rep_spec,
        out_shape=rep_shape,
        scratch_shapes=[tri_scratch],
        name="last",
    )(tri, rep, gate, out_weights)

    other = lax.ppermute(pooled, "tmpl", [(0, 1), (1, 0)])
    return pl.pallas_call(
        functools.partial(finish_kernel, unit),
        grid=(unit // GROUP,),
        in_specs=[
            SMEM,
            whole_block(pooled),
            whole_block(pooled),
            trunk_spec,
            whole_block(coverage),
            whole_block(final_weights),
        ],
        out_specs=trunk_spec,
        out_shape=jax.ShapeDtypeStruct(trunk.shape, BF16),
        scratch_shapes=[pltpu.SMEM((2, unit), jnp.int32), pltpu.VMEM((2 * tile_cols, tile_cols), BF16)],
        name="finish",
    )(coverage, pooled, other, trunk, coverage, final_weights)


def per_device(template_pair, trunk, coverage, *rest):
    unit, _, tile_cols = trunk.shape
    templates, tokens = coverage.shape
    counts = jnp.sum(coverage.reshape(templates, tokens // unit, unit), axis=2)
    capacities = [unit]
    if unit == tile_cols and unit % 16 == 0:
        capacities = [unit * share // 16 for share in (12, 13, 14, 16)]
    args = (counts, template_pair, trunk, coverage) + rest
    if len(capacities) == 1:
        return with_capacity(unit, *args)
    most = jnp.max(counts)
    branch = sum((most > capacity).astype(jnp.int32) for capacity in capacities[:-1])
    return lax.switch(branch, [functools.partial(with_capacity, capacity) for capacity in capacities], *args)


def solution(mesh):
    in_specs = (
        P("tmpl", "row", None, "col"),
        P("row", None, "col"),
        P(),
        P(),
        P(),
        P(),
        P(),
        P(),
        P(),
    )
    out_specs = P("row", None, "col")
    return jax.shard_map(
        per_device, mesh=mesh, in_specs=in_specs, out_specs=out_specs, check_vma=False
    )
```

```python
import functools

import jax
import jax.numpy as jnp
from jax import lax
from jax.experimental import pallas as pl
from jax.experimental.pallas import tpu as pltpu
from jax.sharding import PartitionSpec as P

epsilon = 1e-05
GROUP = 16
F32 = jnp.float32
BF16 = jnp.bfloat16


def sigmoid(x):
    return 0.5 * jnp.tanh(0.5 * x) + 0.5


def norm_rows(x):
    scale = 1.0 / x.shape[0]
    centred = x - jnp.sum(x, axis=0, keepdims=True) * scale
    spread = jnp.sum(centred * centred, axis=0, keepdims=True) * scale
    return centred * lax.rsqrt(spread + epsilon)


def project_rows(weights, rows):
    wide = jnp.concatenate(rows, axis=1)
    out = jnp.dot(weights, wide, preferred_element_type=F32)
    cols = rows[0].shape[1]
    return [out[:, n * cols : (n + 1) * cols] for n in range(len(rows))]


def emit_gated(reps, masks, first, weights_ref, gate_ref, scratch):
    channels = reps[0].shape[0]
    weights = weights_ref[0].reshape(5 * channels, channels)
    normed = [norm_rows(rep).astype(BF16) for rep in reps]
    for half in range(0, len(reps), 2):
        pieces = project_rows(weights, normed[half : half + 2])
        for n, piece in enumerate(pieces):
            p = [piece[k * channels : (k + 1) * channels] for k in range(5)]
            at = first + half + n
            rows = pl.ds(pl.multiple_of(at * (channels + PAD), 8), channels)
            mask = masks[half + n]
            scratch[0, rows, :] = mask * sigmoid(p[0]) * p[1]
            scratch[1, rows, :] = mask * sigmoid(p[2]) * p[3]
            gate_ref[at] = sigmoid(p[4]).astype(gate_ref.dtype)


def packing(capacity, unit, width, per_slot):
    if unit == width:
        for q, p in ((4, 3), (8, 7)):
            if capacity * q <= width * p and 2 * per_slot % q == 0:
                return q, p
    return 1, 1


def lanes_of(shape, dtype=jnp.int32):
    return lax.broadcasted_iota(dtype, shape, len(shape) - 1)


def pack(units, q, p):
    if q == 1:
        return units
    width = units[0].shape[-1]
    kept, piece = width // q * p, width // q
    free = lanes_of(units[0].shape) >= kept
    out = []
    for first in range(0, len(units), q):
        last = units[first + q - 1]
        for e in range(p):
            out.append(jnp.where(free, pltpu.roll(last, kept - e * piece, 1), units[first + e]))
    return out


def unpack_last(packed, q, p):
    width = packed[0].shape[-1]
    piece = width // q
    at = lanes_of(packed[0].shape) // piece
    out = jnp.zeros_like(packed[0])
    for e in range(p):
        out = jnp.where(at == e, pltpu.roll(packed[e], (e + 1) * piece, 1), out)
    return out


def store_by_channel(q, p, scratch, pair_ref):
    slots, units = pair_ref.shape[:2]
    per_slot = units // p * q // 2
    channels = slots * per_slot
    for slot in range(slots):
        values = [
            scratch[side, pl.ds(slot * per_slot + channel, GROUP, stride=channels + PAD), :]
            for side in range(2)
            for channel in range(per_slot)
        ]
        for n, value in enumerate(pack(values, q, p)):
            pair_ref[slot, n] = value.astype(BF16)


STEP = 16
PAD = 8


def block_mask(counts_ref, width, unit):
    template = lax.axis_index("tmpl")
    lanes = lax.broadcasted_iota(jnp.int32, (1, width), 1)
    owners = width // unit
    first = lax.axis_index("col") * owners
    mask = jnp.zeros((1, width), F32)
    for owner in range(owners):
        low = owner * unit
        inside = (lanes >= low) & (lanes < low + counts_ref[template, first + owner])
        mask = jnp.where(inside, 1.0, mask)
    return mask


def selection(cover, unit):
    width = cover.shape[1]
    source = lax.broadcasted_iota(jnp.int32, (width, width), 0)
    target = lax.broadcasted_iota(jnp.int32, (width, width), 1)
    upper = ((source <= target) & (source // unit == target // unit)).astype(F32).astype(BF16)
    wide = jnp.broadcast_to(cover, (GROUP, width)).astype(BF16)
    ranks = jnp.dot(wide, upper, preferred_element_type=F32)[:1].astype(jnp.int32)
    slots = target[:1] // unit * unit + ranks - 1
    return jnp.where((source == slots) & (cover > 0.5), 1.0, 0.0)


def template_row(rows, template):
    out = rows[:1]
    for t in range(1, rows.shape[0]):
        out = jnp.where(template == t, rows[t : t + 1], out)
    return out


def pre_kernel(unit, q, p, cover_ref, chain_ref, counts_ref, tp_hbm, trunk_hbm, cover_all_ref, chain_all_ref, chain_vec_ref,
               trunk_weights_ref, weights_ref, pair_ref, rep_ref, gate_ref,
               scratch, tp_buffer, trunk_buffer, order, pick, sems):
    step_id = pl.program_id(0)
    base = step_id * GROUP
    cols = tp_buffer.shape[3]
    channels = tp_buffer.shape[2]
    template = lax.axis_index("tmpl")
    row_start = lax.axis_index("row") * unit
    col_start = pl.multiple_of(lax.axis_index("col") * cols, cols)
    slot = lax.rem(step_id, 2)

    def copies(group, into):
        out = []
        for n in range(GROUP):
            row = order[group * GROUP + n]
            out.append(pltpu.make_async_copy(tp_hbm.at[0, row], tp_buffer.at[into, n], sems.at[into, 0, n]))
            out.append(pltpu.make_async_copy(trunk_hbm.at[row], trunk_buffer.at[into, n], sems.at[into, 1, n]))
        return out

    @pl.when(step_id == 0)
    def _():
        def place(row, taken):
            covered = cover_ref[template, row_start + row]
            order[jnp.where(covered > 0, taken, unit - 1 - (row - taken))] = row
            return taken + covered

        lax.fori_loop(0, unit, place, 0, unroll=8)
        for copy in copies(0, 0):
            copy.start()
        cover = template_row(cover_all_ref[:, pl.ds(col_start, cols)].astype(F32), template)
        pick[...] = jnp.transpose(selection(cover, unit)).astype(BF16)

    @pl.when(step_id + 1 < pl.num_programs(0))
    def _():
        for copy in copies(step_id + 1, 1 - slot):
            copy.start()

    for copy in copies(step_id, slot):
        copy.wait()

    trunk_weights = trunk_weights_ref[...]
    weight_sums = jnp.sum(trunk_weights.astype(F32), axis=1, keepdims=True)
    diagonal = lax.broadcasted_iota(jnp.int32, (channels, channels), 0) == lanes_of((channels, channels))
    chain_column = jnp.sum(jnp.where(diagonal, chain_vec_ref[...], 0.0), axis=1, keepdims=True)
    chain_cols = chain_all_ref[:, pl.ds(col_start, cols)]
    col_mask = block_mask(counts_ref, cols, unit)
    row_count = counts_ref[template, lax.axis_index("row")]

    def body(step, carry):
        first = step * STEP
        raw, masks = [], []
        rows = [trunk_buffer[slot, first + n] for n in range(STEP)]
        projected = []
        for half in range(0, STEP, 2):
            projected += project_rows(trunk_weights, rows[half : half + 2])
        for n in range(STEP):
            at = first + n
            values = rows[n].astype(F32)
            scale = 1.0 / values.shape[0]
            centre = jnp.sum(values, axis=0, keepdims=True) * scale
            centred = values - centre
            spread = jnp.sum(centred * centred, axis=0, keepdims=True) * scale
            trunk_proj = (projected[n] - weight_sums * centre) * lax.rsqrt(spread + epsilon)
            same = (chain_cols == chain_ref[row_start + order[base + at]]).astype(F32)
            raw.append((tp_buffer[slot, at].astype(F32) + same * chain_column + trunk_proj).astype(BF16))
            masks.append(jnp.where(base + at < row_count, col_mask, 0.0))
        picked = jnp.dot(jnp.concatenate(raw, axis=0), pick[...], preferred_element_type=F32)
        reps = [picked[n * channels : (n + 1) * channels] for n in range(STEP)]
        for n in range(STEP):
            rep_ref[first + n] = reps[n].astype(BF16)
        emit_gated(reps, masks, first, weights_ref, gate_ref, scratch)
        return carry

    lax.fori_loop(0, GROUP // STEP, body, 0)
    store_by_channel(q, p, scratch, pair_ref)


def returned_rows(capacity, per_slot, q):
    if q == 1:
        return per_slot * capacity
    left = per_slot - 1
    return left * capacity + (8 * pl.cdiv(capacity, 16) if left < q - 1 else 0)


def load_tri(capacity, q, tri_ref, tri_scratch):
    slots, _, width = tri_ref.shape
    channels = tri_scratch.shape[0] // (GROUP + PAD)
    per_slot = channels // slots
    scale = 1.0 / channels
    base = pl.program_id(0) * GROUP
    total = jnp.zeros((GROUP, width), F32)
    whole = per_slot if q == 1 else per_slot - 1
    piece = width // q
    lanes = lanes_of((GROUP, width))
    for slot in range(slots):
        units = [
            tri_ref[slot, pl.ds(pl.multiple_of(e * capacity + base, 8), GROUP), :].astype(F32) for e in range(whole)
        ]
        if whole < per_slot:
            last = jnp.zeros_like(total)
            for e in range(whole):
                last = jnp.where(lanes // piece == e, pltpu.roll(units[e], (e + 1) * piece, 1), last)
            if whole < q - 1:
                start = whole * piece
                half = (width - piece - start) % width
                at = pl.multiple_of(whole * capacity + pl.program_id(0) * 8, 8)
                folded = tri_ref[slot, pl.ds(at, 8), :].astype(F32)
                rest = jnp.concatenate(
                    [pltpu.roll(folded, start, 1), pltpu.roll(folded, width + start - half, 1)], axis=0
                )
                last = jnp.where(lanes < start, last, rest)
            units.append(last)
        for e, value in enumerate(units):
            at = (slot * per_slot + e) * (GROUP + PAD)
            tri_scratch[at : at + GROUP, :] = value
            total += value
    centre = total * scale
    total = jnp.zeros_like(total)
    for channel in range(channels):
        at = channel * (GROUP + PAD)
        centred = tri_scratch[at : at + GROUP, :] - centre
        total += centred * centred
    inverse = lax.rsqrt(total * scale + epsilon)
    for channel in range(channels):
        at = channel * (GROUP + PAD)
        tri_scratch[at : at + GROUP, :] = (tri_scratch[at : at + GROUP, :] - centre) * inverse


def updated_rows(first, tri_scratch, rep_ref, gate_ref, out_weights_ref):
    channels = rep_ref.shape[1]
    normed = [
        tri_scratch[pl.ds(first + n, channels, stride=GROUP + PAD), :].astype(BF16) for n in range(STEP)
    ]
    projected = []
    for half in range(0, STEP, 2):
        projected += project_rows(out_weights_ref[0], normed[half : half + 2])
    return [
        (rep_ref[first + n].astype(F32) + gate_ref[first + n].astype(F32) * projected[n]).astype(BF16)
        for n in range(STEP)
    ]


def mid_kernel(unit, capacity, q, p, counts_ref, tri_ref, rep_in_ref, gate_in_ref, out_weights_ref, weights_ref,
               pair_ref, rep_ref, gate_ref, scratch, tri_scratch):
    base = pl.program_id(0) * GROUP
    load_tri(capacity, q, tri_ref, tri_scratch)
    col_mask = block_mask(counts_ref, rep_ref.shape[2], unit)
    row_count = counts_ref[lax.axis_index("tmpl"), lax.axis_index("row")]

    def body(step, carry):
        first = step * STEP
        rows = updated_rows(first, tri_scratch, rep_in_ref, gate_in_ref, out_weights_ref)
        masks = []
        for n in range(STEP):
            rep_ref[first + n] = rows[n]
            masks.append(jnp.where(base + first + n < row_count, col_mask, 0.0))
        emit_gated([row.astype(F32) for row in rows], masks, first, weights_ref, gate_ref, scratch)
        return carry

    lax.fori_loop(0, GROUP // STEP, body, 0)
    store_by_channel(q, p, scratch, pair_ref)


def last_kernel(capacity, q, tri_ref, rep_in_ref, gate_in_ref, out_weights_ref, pooled_ref, tri_scratch):
    load_tri(capacity, q, tri_ref, tri_scratch)

    def body(step, carry):
        first = step * STEP
        rows = updated_rows(first, tri_scratch, rep_in_ref, gate_in_ref, out_weights_ref)
        for n in range(STEP):
            pooled_ref[first + n] = norm_rows(rows[n].astype(F32)).astype(BF16)
        return carry

    lax.fori_loop(0, GROUP // STEP, body, 0)


def finish_kernel(unit, cover_ref, mine_ref, other_ref, trunk_ref, cover_all_ref, final_weights_ref, out_ref,
                  place, spread):
    step_id = pl.program_id(0)
    group, _, cols = out_ref.shape
    base = step_id * group
    channels = mine_ref.shape[1]
    template = lax.axis_index("tmpl")
    templates = (template, 1 - template)
    row_start = lax.axis_index("row") * unit
    col_start = pl.multiple_of(lax.axis_index("col") * cols, cols)
    cover_cols = cover_all_ref[:, pl.ds(col_start, cols)].astype(F32)
    covers = [template_row(cover_cols, t) for t in templates]

    @pl.when(step_id == 0)
    def _():
        def count(row, taken):
            out = []
            for k, t in enumerate(templates):
                covered = cover_ref[t, row_start + row]
                place[k, row] = jnp.where(covered > 0, taken[k], 0)
                out.append(taken[k] + covered)
            return tuple(out)

        lax.fori_loop(0, unit, count, (0,) * len(templates), unroll=8)
        for k in range(len(templates)):
            spread[k * cols : (k + 1) * cols, :] = selection(covers[k], unit).astype(BF16)

    def body(step, carry):
        first = step * group
        packed, counts = [], []
        for n in range(group):
            row = base + first + n
            parts = []
            count = jnp.zeros_like(covers[0])
            for k, (t, ref) in enumerate(zip(templates, (mine_ref, other_ref))):
                covered = cover_ref[t, row_start + row]
                value = ref[place[k, row]]
                parts.append(lax.select(covered > 0, value, jnp.zeros_like(value)))
                count += covers[k] * covered.astype(F32)
            packed.append(jnp.concatenate(parts, axis=1))
            counts.append(count)
        pooled = jnp.dot(jnp.concatenate(packed, axis=0), spread[...], preferred_element_type=F32)
        hidden = [
            jnp.maximum(pooled[n * channels : (n + 1) * channels] * (1.0 / jnp.maximum(counts[n], 1.0)), 0.0).astype(BF16)
            for n in range(group)
        ]
        for half in range(0, group, 2):
            for n, row in enumerate(project_rows(final_weights_ref[...], hidden[half : half + 2])):
                at = first + half + n
                out_ref[at] = (trunk_ref[at].astype(F32) + row).astype(BF16)
        return carry

    body(0, 0)


def gather_sides(rows_n, cols_n, unit, q, p, pair_ref, sides):
    units, height, width = pair_ref.shape[1:]
    per_slot = units // p * q // 2
    channel = per_slot - 1 - pl.program_id(0)

    @pl.when(pl.program_id(0) == 0)
    def _():
        if height < unit:
            sides[...] = jnp.zeros_like(sides)

    keep = (lanes_of((1, width)) < width // q * p).astype(F32).astype(BF16)
    for side in range(2):
        index = side * per_slot + channel
        first = index // q * p

        def fill(block, side=side):
            def fill_rows(r, carry):
                rows = pl.ds(pl.multiple_of(r * unit, unit), height)
                for c in range(cols_n):
                    sides[side, rows, c * width : (c + 1) * width] = block(r * cols_n + c)
                return carry

            lax.fori_loop(0, rows_n, fill_rows, 0)

        if q == 1:
            fill(lambda slot, index=index: pair_ref[slot, index])
            continue

        @pl.when(lax.rem(index, q) < p)
        def _(fill=fill, index=index, first=first):
            fill(lambda slot: pair_ref[slot, first + lax.rem(index, q)] * keep)

        if (side + 1) * per_slot % q == 0:

            @pl.when(lax.rem(index, q) == p)
            def _(fill=fill, first=first):
                fill(
                    lambda slot: unpack_last(
                        [pair_ref[slot, first + e].astype(F32) for e in range(p)], q, p
                    ).astype(BF16)
                )


def triangle_kernel(contract, rows_n, cols_n, unit, q, p, pair_ref, tri_ref, sides, cut):
    gather_sides(rows_n, cols_n, unit, q, p, pair_ref, sides)
    out = lax.dot_general(
        sides[0], sides[1], (((contract,), (contract,)), ((), ())), preferred_element_type=F32
    )
    capacity, width = pair_ref.shape[2:]
    per_slot = pair_ref.shape[1] // p * q // 2
    channel = per_slot - 1 - pl.program_id(0)
    blocks = [
        (r * cols_n + c, out[r * unit : (r + 1) * unit, c * width : (c + 1) * width])
        for r in range(rows_n)
        for c in range(cols_n)
    ]
    place = pl.ds(pl.multiple_of(channel * capacity, 8), capacity)
    if q == 1:
        for slot, block in blocks:
            tri_ref[slot, place, :] = block[:capacity].astype(BF16)
        return

    piece = width // q
    kept = width - piece

    @pl.when(channel == per_slot - 1)
    def _():
        whole = per_slot - 1
        start = whole * piece
        folds = tri_ref.shape[1] - whole * capacity
        for slot, block in blocks:
            cut[slot] = block[:capacity]
            if folds:
                half = kept - start
                tiles = block[: 2 * folds].reshape(folds // 8, 2, 8, width)
                first = tiles[:, 0].reshape(folds, width)
                second = tiles[:, 1].reshape(folds, width)
                folded = jnp.where(
                    lanes_of(first.shape) < half,
                    pltpu.roll(first, width - start, 1),
                    pltpu.roll(second, (half - start) % width, 1),
                )
                tri_ref[slot, whole * capacity :, :] = folded.astype(BF16)

    @pl.when(channel < per_slot - 1)
    def _():
        for slot, block in blocks:
            free = lanes_of((capacity, width)) >= kept
            moved = pltpu.roll(cut[slot], kept - channel * piece, 1)
            tri_ref[slot, place, :] = jnp.where(free, moved, block[:capacity]).astype(BF16)


def triangle(contract, rows_n, cols_n, unit, q, p, pairs, name):
    slots, units, capacity, width = pairs.shape
    per_slot = units // p * q // 2
    shape = (slots, returned_rows(capacity, per_slot, q), width)
    cut = (slots, capacity, width) if q > 1 else (1, 8, width)
    return pl.pallas_call(
        functools.partial(triangle_kernel, contract, rows_n, cols_n, unit, q, p),
        grid=(per_slot,),
        in_specs=[pl.BlockSpec(pairs.shape, lambda c: (0, 0, 0, 0))],
        out_specs=pl.BlockSpec(shape, lambda c: (0, 0, 0)),
        out_shape=jax.ShapeDtypeStruct(shape, BF16),
        scratch_shapes=[pltpu.VMEM((2, rows_n * unit, cols_n * width), BF16), pltpu.VMEM(cut, F32)],
        name=name,
    )(pairs)


SMEM = pl.BlockSpec(memory_space=pltpu.SMEM)
ANY = pl.BlockSpec(memory_space=pl.ANY)


def whole_block(array):
    zeros = (0,) * array.ndim
    return pl.BlockSpec(array.shape, lambda g: zeros)


def update_block(array, number):
    index = (number,) + (0,) * (array.ndim - 1)
    return pl.BlockSpec((1,) + array.shape[1:], lambda g: index)


def rows_block(*rest):
    zeros = (0,) * len(rest)
    return pl.BlockSpec((GROUP,) + rest, lambda g: (g,) + zeros)


def with_capacity(
    capacity,
    counts,
    template_pair,
    trunk,
    coverage,
    chain_ids,
    chain_vec,
    trunk_weights,
    proj_weights,
    out_weights,
    final_weights,
):
    unit, trunk_channels, tile_cols = trunk.shape
    channels = template_pair.shape[2]
    rows_n, cols_n = lax.axis_size("row"), lax.axis_size("col")
    slots = rows_n * cols_n
    per_slot = channels // slots
    grid = (pl.cdiv(capacity, GROUP),)
    q, p = packing(capacity, unit, tile_cols, per_slot)
    chain_all = chain_ids[None]
    chain_row = chain_vec[None]

    units = 2 * per_slot // q * p
    pair_spec = pl.BlockSpec((slots, units, GROUP, tile_cols), lambda g: (0, 0, g, 0))
    pair_shape = jax.ShapeDtypeStruct((slots, units, capacity, tile_cols), BF16)
    rep_spec = rows_block(channels, tile_cols)
    rep_shape = jax.ShapeDtypeStruct((capacity, channels, tile_cols), BF16)
    finish_rows = 2 * GROUP if unit % (2 * GROUP) == 0 else GROUP
    finish_spec = pl.BlockSpec((finish_rows, trunk_channels, tile_cols), lambda g: (g, 0, 0))
    tri_spec = pl.BlockSpec((slots, returned_rows(capacity, per_slot, q), tile_cols), lambda g: (0, 0, 0))
    scratch = pltpu.VMEM((2, GROUP * (channels + PAD), tile_cols), F32)
    tri_scratch = pltpu.VMEM((channels * (GROUP + PAD), tile_cols), F32)
    gated_outs = dict(
        out_specs=[pair_spec, rep_spec, rep_spec], out_shape=[pair_shape, rep_shape, rep_shape]
    )

    def exchange(values):
        return lax.all_to_all(values, ("row", "col"), 0, 0, tiled=True)

    pairs, rep, gate = pl.pallas_call(
        functools.partial(pre_kernel, unit, q, p),
        grid=grid,
        in_specs=[
            SMEM,
            SMEM,
            SMEM,
            ANY,
            ANY,
            whole_block(coverage),
            whole_block(chain_all),
            whole_block(chain_row),
            whole_block(trunk_weights),
            update_block(proj_weights, 0),
        ],
        scratch_shapes=[
            scratch,
            pltpu.VMEM((2, GROUP, channels, tile_cols), BF16),
            pltpu.VMEM((2, GROUP, trunk_channels, tile_cols), BF16),
            pltpu.SMEM((unit,), jnp.int32),
            pltpu.VMEM((tile_cols, tile_cols), BF16),
            pltpu.SemaphoreType.DMA((2, 2, GROUP)),
        ],
        name="pre",
        **gated_outs,
    )(coverage, chain_ids, counts, template_pair, trunk, coverage, chain_all, chain_row, trunk_weights, proj_weights)

    tri = exchange(triangle(1, rows_n, cols_n, unit, q, p, exchange(pairs), "outgoing"))
    pairs, rep, gate = pl.pallas_call(
        functools.partial(mid_kernel, unit, capacity, q, p),
        grid=grid,
        in_specs=[SMEM, tri_spec, rep_spec, rep_spec, update_block(out_weights, 0), update_block(proj_weights, 1)],
        scratch_shapes=[scratch, tri_scratch],
        name="mid",
        **gated_outs,
    )(counts, tri, rep, gate, out_weights, proj_weights)

    tri = exchange(triangle(0, rows_n, cols_n, unit, q, p, exchange(pairs), "incoming"))
    pooled = pl.pallas_call(
        functools.partial(last_kernel, capacity, q),
        grid=grid,
        in_specs=[tri_spec, rep_spec, rep_spec, update_block(out_weights, 1)],
        out_specs=rep_spec,
        out_shape=rep_shape,
        scratch_shapes=[tri_scratch],
        name="last",
    )(tri, rep, gate, out_weights)

    other = lax.ppermute(pooled, "tmpl", [(0, 1), (1, 0)])
    return pl.pallas_call(
        functools.partial(finish_kernel, unit),
        grid=(unit // finish_rows,),
        in_specs=[
            SMEM,
            whole_block(pooled),
            whole_block(pooled),
            finish_spec,
            whole_block(coverage),
            whole_block(final_weights),
        ],
        out_specs=finish_spec,
        out_shape=jax.ShapeDtypeStruct(trunk.shape, BF16),
        scratch_shapes=[pltpu.SMEM((2, unit), jnp.int32), pltpu.VMEM((2 * tile_cols, tile_cols), BF16)],
        name="finish",
    )(coverage, pooled, other, trunk, coverage, final_weights)


def per_device(template_pair, trunk, coverage, *rest):
    unit, _, tile_cols = trunk.shape
    templates, tokens = coverage.shape
    counts = jnp.sum(coverage.reshape(templates, tokens // unit, unit), axis=2)
    capacities = [unit]
    if unit == tile_cols and unit % 16 == 0:
        capacities = [unit * share // 16 for share in (12, 13, 14, 16)]
    args = (counts, template_pair, trunk, coverage) + rest
    if len(capacities) == 1:
        return with_capacity(unit, *args)
    most = jnp.max(counts)
    branch = sum((most > capacity).astype(jnp.int32) for capacity in capacities[:-1])
    return lax.switch(branch, [functools.partial(with_capacity, capacity) for capacity in capacities], *args)


def solution(mesh):
    in_specs = (
        P("tmpl", "row", None, "col"),
        P("row", None, "col"),
        P(),
        P(),
        P(),
        P(),
        P(),
        P(),
        P(),
    )
    out_specs = P("row", None, "col")
    return jax.shard_map(
        per_device, mesh=mesh, in_specs=in_specs, out_specs=out_specs, check_vma=False
    )
```

```python
import functools

import jax
import jax.numpy as jnp
from jax import lax
from jax.experimental import pallas as pl
from jax.experimental.pallas import tpu as pltpu
from jax.sharding import PartitionSpec as P

epsilon = 1e-05
GROUP = 16
F32 = jnp.float32
BF16 = jnp.bfloat16


def sigmoid(x):
    return 0.5 * jnp.tanh(0.5 * x) + 0.5


def norm_rows(x):
    scale = 1.0 / x.shape[0]
    centred = x - jnp.sum(x, axis=0, keepdims=True) * scale
    spread = jnp.sum(centred * centred, axis=0, keepdims=True) * scale
    return centred * lax.rsqrt(spread + epsilon)


def project_rows(weights, rows):
    wide = jnp.concatenate(rows, axis=1)
    out = jnp.dot(weights, wide, preferred_element_type=F32)
    cols = rows[0].shape[1]
    return [out[:, n * cols : (n + 1) * cols] for n in range(len(rows))]


def emit_gated(reps, masks, first, weights_ref, gate_ref, scratch):
    channels = reps[0].shape[0]
    weights = weights_ref[0].reshape(5 * channels, channels)
    normed = [norm_rows(rep).astype(BF16) for rep in reps]
    for half in range(0, len(reps), 2):
        pieces = project_rows(weights, normed[half : half + 2])
        for n, piece in enumerate(pieces):
            p = [piece[k * channels : (k + 1) * channels] for k in range(5)]
            at = first + half + n
            rows = pl.ds(pl.multiple_of(at * (channels + PAD), 8), channels)
            mask = masks[half + n]
            scratch[0, rows, :] = mask * sigmoid(p[0]) * p[1]
            scratch[1, rows, :] = mask * sigmoid(p[2]) * p[3]
            gate_ref[at] = sigmoid(p[4]).astype(gate_ref.dtype)


def packing(capacity, unit, width, per_slot):
    if unit == width:
        for q, p in ((4, 3), (8, 7)):
            if capacity * q <= width * p and 2 * per_slot % q == 0:
                return q, p
    return 1, 1


def lanes_of(shape, dtype=jnp.int32):
    return lax.broadcasted_iota(dtype, shape, len(shape) - 1)


def pack(units, q, p):
    if q == 1:
        return units
    width = units[0].shape[-1]
    kept, piece = width // q * p, width // q
    free = lanes_of(units[0].shape) >= kept
    out = []
    for first in range(0, len(units), q):
        last = units[first + q - 1]
        for e in range(p):
            out.append(jnp.where(free, pltpu.roll(last, kept - e * piece, 1), units[first + e]))
    return out


def unpack_last(packed, q, p):
    width = packed[0].shape[-1]
    piece = width // q
    at = lanes_of(packed[0].shape) // piece
    out = jnp.zeros_like(packed[0])
    for e in range(p):
        out = jnp.where(at == e, pltpu.roll(packed[e], (e + 1) * piece, 1), out)
    return out


def store_by_channel(q, p, scratch, pair_ref):
    slots, units = pair_ref.shape[:2]
    per_slot = units // p * q // 2
    channels = slots * per_slot
    for slot in range(slots):
        values = [
            scratch[side, pl.ds(slot * per_slot + channel, GROUP, stride=channels + PAD), :]
            for side in range(2)
            for channel in range(per_slot)
        ]
        for n, value in enumerate(pack(values, q, p)):
            pair_ref[slot, n] = value.astype(BF16)


STEP = 16
PAD = 8


def block_mask(counts_ref, width, unit):
    template = lax.axis_index("tmpl")
    lanes = lax.broadcasted_iota(jnp.int32, (1, width), 1)
    owners = width // unit
    first = lax.axis_index("col") * owners
    mask = jnp.zeros((1, width), F32)
    for owner in range(owners):
        low = owner * unit
        inside = (lanes >= low) & (lanes < low + counts_ref[template, first + owner])
        mask = jnp.where(inside, 1.0, mask)
    return mask


def selection(cover, unit):
    width = cover.shape[1]
    source = lax.broadcasted_iota(jnp.int32, (width, width), 0)
    target = lax.broadcasted_iota(jnp.int32, (width, width), 1)
    upper = ((source <= target) & (source // unit == target // unit)).astype(F32).astype(BF16)
    wide = jnp.broadcast_to(cover, (GROUP, width)).astype(BF16)
    ranks = jnp.dot(wide, upper, preferred_element_type=F32)[:1].astype(jnp.int32)
    slots = target[:1] // unit * unit + ranks - 1
    return jnp.where((source == slots) & (cover > 0.5), 1.0, 0.0)


def template_row(rows, template):
    out = rows[:1]
    for t in range(1, rows.shape[0]):
        out = jnp.where(template == t, rows[t : t + 1], out)
    return out


def pre_kernel(unit, q, p, cover_ref, chain_ref, counts_ref, tp_hbm, trunk_hbm, cover_all_ref, chain_all_ref, chain_vec_ref,
               trunk_weights_ref, weights_ref, pair_ref, rep_ref, gate_ref,
               scratch, tp_buffer, trunk_buffer, order, pick, sems):
    step_id = pl.program_id(0)
    base = step_id * GROUP
    cols = tp_buffer.shape[3]
    channels = tp_buffer.shape[2]
    template = lax.axis_index("tmpl")
    row_start = lax.axis_index("row") * unit
    col_start = pl.multiple_of(lax.axis_index("col") * cols, cols)
    slot = lax.rem(step_id, 2)

    def copies(group, into):
        out = []
        for n in range(GROUP):
            row = order[group * GROUP + n]
            out.append(pltpu.make_async_copy(tp_hbm.at[0, row], tp_buffer.at[into, n], sems.at[into, 0, n]))
            out.append(pltpu.make_async_copy(trunk_hbm.at[row], trunk_buffer.at[into, n], sems.at[into, 1, n]))
        return out

    @pl.when(step_id == 0)
    def _():
        def place(row, taken):
            covered = cover_ref[template, row_start + row]
            order[jnp.where(covered > 0, taken, unit - 1 - (row - taken))] = row
            return taken + covered

        lax.fori_loop(0, unit, place, 0, unroll=32)
        for copy in copies(0, 0):
            copy.start()
        cover = template_row(cover_all_ref[:, pl.ds(col_start, cols)].astype(F32), template)
        pick[...] = jnp.transpose(selection(cover, unit)).astype(BF16)

    @pl.when(step_id + 1 < pl.num_programs(0))
    def _():
        for copy in copies(step_id + 1, 1 - slot):
            copy.start()

    for copy in copies(step_id, slot):
        copy.wait()

    trunk_weights = trunk_weights_ref[...]
    weight_sums = jnp.sum(trunk_weights.astype(F32), axis=1, keepdims=True)
    diagonal = lax.broadcasted_iota(jnp.int32, (channels, channels), 0) == lanes_of((channels, channels))
    chain_column = jnp.sum(jnp.where(diagonal, chain_vec_ref[...], 0.0), axis=1, keepdims=True)
    chain_cols = chain_all_ref[:, pl.ds(col_start, cols)]
    col_mask = block_mask(counts_ref, cols, unit)
    row_count = counts_ref[template, lax.axis_index("row")]

    def body(step, carry):
        first = step * STEP
        raw, masks = [], []
        rows = [trunk_buffer[slot, first + n] for n in range(STEP)]
        projected = []
        for half in range(0, STEP, 2):
            projected += project_rows(trunk_weights, rows[half : half + 2])
        for n in range(STEP):
            at = first + n
            values = rows[n].astype(F32)
            scale = 1.0 / values.shape[0]
            centre = jnp.sum(values, axis=0, keepdims=True) * scale
            centred = values - centre
            spread = jnp.sum(centred * centred, axis=0, keepdims=True) * scale
            trunk_proj = (projected[n] - weight_sums * centre) * lax.rsqrt(spread + epsilon)
            same = (chain_cols == chain_ref[row_start + order[base + at]]).astype(F32)
            raw.append((tp_buffer[slot, at].astype(F32) + same * chain_column + trunk_proj).astype(BF16))
            masks.append(jnp.where(base + at < row_count, col_mask, 0.0))
        picked = jnp.dot(jnp.concatenate(raw, axis=0), pick[...], preferred_element_type=F32)
        reps = [picked[n * channels : (n + 1) * channels] for n in range(STEP)]
        for n in range(STEP):
            rep_ref[first + n] = reps[n].astype(BF16)
        emit_gated(reps, masks, first, weights_ref, gate_ref, scratch)
        return carry

    lax.fori_loop(0, GROUP // STEP, body, 0)
    store_by_channel(q, p, scratch, pair_ref)


def returned_rows(capacity, per_slot, q):
    if q == 1:
        return per_slot * capacity
    left = per_slot - 1
    return left * capacity + (8 * pl.cdiv(capacity, 16) if left < q - 1 else 0)


def load_tri(capacity, q, tri_ref, tri_scratch):
    slots, _, width = tri_ref.shape
    channels = tri_scratch.shape[0] // (GROUP + PAD)
    per_slot = channels // slots
    scale = 1.0 / channels
    base = pl.program_id(0) * GROUP
    total = jnp.zeros((GROUP, width), F32)
    whole = per_slot if q == 1 else per_slot - 1
    piece = width // q
    lanes = lanes_of((GROUP, width))
    for slot in range(slots):
        units = [
            tri_ref[slot, pl.ds(pl.multiple_of(e * capacity + base, 8), GROUP), :].astype(F32) for e in range(whole)
        ]
        if whole < per_slot:
            last = jnp.zeros_like(total)
            for e in range(whole):
                last = jnp.where(lanes // piece == e, pltpu.roll(units[e], (e + 1) * piece, 1), last)
            if whole < q - 1:
                start = whole * piece
                half = (width - piece - start) % width
                at = pl.multiple_of(whole * capacity + pl.program_id(0) * 8, 8)
                folded = tri_ref[slot, pl.ds(at, 8), :].astype(F32)
                rest = jnp.concatenate(
                    [pltpu.roll(folded, start, 1), pltpu.roll(folded, width + start - half, 1)], axis=0
                )
                last = jnp.where(lanes < start, last, rest)
            units.append(last)
        for e, value in enumerate(units):
            at = (slot * per_slot + e) * (GROUP + PAD)
            tri_scratch[at : at + GROUP, :] = value
            total += value
    centre = total * scale
    total = jnp.zeros_like(total)
    for channel in range(channels):
        at = channel * (GROUP + PAD)
        centred = tri_scratch[at : at + GROUP, :] - centre
        total += centred * centred
    inverse = lax.rsqrt(total * scale + epsilon)
    for channel in range(channels):
        at = channel * (GROUP + PAD)
        tri_scratch[at : at + GROUP, :] = (tri_scratch[at : at + GROUP, :] - centre) * inverse


def updated_rows(first, tri_scratch, rep_ref, gate_ref, out_weights_ref):
    channels = rep_ref.shape[1]
    normed = [
        tri_scratch[pl.ds(first + n, channels, stride=GROUP + PAD), :].astype(BF16) for n in range(STEP)
    ]
    projected = []
    for half in range(0, STEP, 2):
        projected += project_rows(out_weights_ref[0], normed[half : half + 2])
    return [
        (rep_ref[first + n].astype(F32) + gate_ref[first + n].astype(F32) * projected[n]).astype(BF16)
        for n in range(STEP)
    ]


def mid_kernel(unit, capacity, q, p, counts_ref, tri_ref, rep_in_ref, gate_in_ref, out_weights_ref, weights_ref,
               pair_ref, rep_ref, gate_ref, scratch, tri_scratch):
    base = pl.program_id(0) * GROUP
    load_tri(capacity, q, tri_ref, tri_scratch)
    col_mask = block_mask(counts_ref, rep_ref.shape[2], unit)
    row_count = counts_ref[lax.axis_index("tmpl"), lax.axis_index("row")]

    def body(step, carry):
        first = step * STEP
        rows = updated_rows(first, tri_scratch, rep_in_ref, gate_in_ref, out_weights_ref)
        masks = []
        for n in range(STEP):
            rep_ref[first + n] = rows[n]
            masks.append(jnp.where(base + first + n < row_count, col_mask, 0.0))
        emit_gated([row.astype(F32) for row in rows], masks, first, weights_ref, gate_ref, scratch)
        return carry

    lax.fori_loop(0, GROUP // STEP, body, 0)
    store_by_channel(q, p, scratch, pair_ref)


def last_kernel(capacity, q, tri_ref, rep_in_ref, gate_in_ref, out_weights_ref, pooled_ref, tri_scratch):
    load_tri(capacity, q, tri_ref, tri_scratch)

    def body(step, carry):
        first = step * STEP
        rows = updated_rows(first, tri_scratch, rep_in_ref, gate_in_ref, out_weights_ref)
        for n in range(STEP):
            pooled_ref[first + n] = norm_rows(rows[n].astype(F32)).astype(BF16)
        return carry

    lax.fori_loop(0, GROUP // STEP, body, 0)


def finish_kernel(unit, cover_ref, mine_ref, other_ref, trunk_ref, cover_all_ref, final_weights_ref, out_ref,
                  place, spread):
    step_id = pl.program_id(0)
    group, _, cols = out_ref.shape
    base = step_id * group
    channels = mine_ref.shape[1]
    template = lax.axis_index("tmpl")
    templates = (template, 1 - template)
    row_start = lax.axis_index("row") * unit
    col_start = pl.multiple_of(lax.axis_index("col") * cols, cols)
    cover_cols = cover_all_ref[:, pl.ds(col_start, cols)].astype(F32)
    covers = [template_row(cover_cols, t) for t in templates]

    @pl.when(step_id == 0)
    def _():
        def count(row, taken):
            out = []
            for k, t in enumerate(templates):
                covered = cover_ref[t, row_start + row]
                place[k, row] = jnp.where(covered > 0, taken[k], 0)
                out.append(taken[k] + covered)
            return tuple(out)

        lax.fori_loop(0, unit, count, (0,) * len(templates), unroll=32)
        for k in range(len(templates)):
            spread[k * cols : (k + 1) * cols, :] = selection(covers[k], unit).astype(BF16)

    def body(step, carry):
        first = step * group
        packed, counts = [], []
        for n in range(group):
            row = base + first + n
            parts = []
            count = jnp.zeros_like(covers[0])
            for k, (t, ref) in enumerate(zip(templates, (mine_ref, other_ref))):
                covered = cover_ref[t, row_start + row]
                value = ref[place[k, row]]
                parts.append(lax.select(covered > 0, value, jnp.zeros_like(value)))
                count += covers[k] * covered.astype(F32)
            packed.append(jnp.concatenate(parts, axis=1))
            counts.append(count)
        pooled = jnp.dot(jnp.concatenate(packed, axis=0), spread[...], preferred_element_type=F32)
        hidden = [
            jnp.maximum(pooled[n * channels : (n + 1) * channels] * (1.0 / jnp.maximum(counts[n], 1.0)), 0.0).astype(BF16)
            for n in range(group)
        ]
        for half in range(0, group, 2):
            for n, row in enumerate(project_rows(final_weights_ref[...], hidden[half : half + 2])):
                at = first + half + n
                out_ref[at] = (trunk_ref[at].astype(F32) + row).astype(BF16)
        return carry

    body(0, 0)


def gather_sides(rows_n, cols_n, unit, q, p, pair_ref, sides):
    units, height, width = pair_ref.shape[1:]
    per_slot = units // p * q // 2
    channel = per_slot - 1 - pl.program_id(0)

    @pl.when(pl.program_id(0) == 0)
    def _():
        if height < unit:
            sides[...] = jnp.zeros_like(sides)

    keep = (lanes_of((1, width)) < width // q * p).astype(F32).astype(BF16)
    for side in range(2):
        index = side * per_slot + channel
        first = index // q * p

        def fill(block, side=side):
            def fill_rows(r, carry):
                rows = pl.ds(pl.multiple_of(r * unit, unit), height)
                for c in range(cols_n):
                    sides[side, rows, c * width : (c + 1) * width] = block(r * cols_n + c)
                return carry

            lax.fori_loop(0, rows_n, fill_rows, 0)

        if q == 1:
            fill(lambda slot, index=index: pair_ref[slot, index])
            continue

        @pl.when(lax.rem(index, q) < p)
        def _(fill=fill, index=index, first=first):
            fill(lambda slot: pair_ref[slot, first + lax.rem(index, q)] * keep)

        if (side + 1) * per_slot % q == 0:

            @pl.when(lax.rem(index, q) == p)
            def _(fill=fill, first=first):
                fill(
                    lambda slot: unpack_last(
                        [pair_ref[slot, first + e].astype(F32) for e in range(p)], q, p
                    ).astype(BF16)
                )


def triangle_kernel(contract, rows_n, cols_n, unit, q, p, pair_ref, tri_ref, sides, cut):
    gather_sides(rows_n, cols_n, unit, q, p, pair_ref, sides)
    out = lax.dot_general(
        sides[0], sides[1], (((contract,), (contract,)), ((), ())), preferred_element_type=F32
    )
    capacity, width = pair_ref.shape[2:]
    per_slot = pair_ref.shape[1] // p * q // 2
    channel = per_slot - 1 - pl.program_id(0)
    blocks = [
        (r * cols_n + c, out[r * unit : (r + 1) * unit, c * width : (c + 1) * width])
        for r in range(rows_n)
        for c in range(cols_n)
    ]
    place = pl.ds(pl.multiple_of(channel * capacity, 8), capacity)
    if q == 1:
        for slot, block in blocks:
            tri_ref[slot, place, :] = block[:capacity].astype(BF16)
        return

    piece = width // q
    kept = width - piece

    @pl.when(channel == per_slot - 1)
    def _():
        whole = per_slot - 1
        start = whole * piece
        folds = tri_ref.shape[1] - whole * capacity
        for slot, block in blocks:
            cut[slot] = block[:capacity]
            if folds:
                half = kept - start
                tiles = block[: 2 * folds].reshape(folds // 8, 2, 8, width)
                first = tiles[:, 0].reshape(folds, width)
                second = tiles[:, 1].reshape(folds, width)
                folded = jnp.where(
                    lanes_of(first.shape) < half,
                    pltpu.roll(first, width - start, 1),
                    pltpu.roll(second, (half - start) % width, 1),
                )
                tri_ref[slot, whole * capacity :, :] = folded.astype(BF16)

    @pl.when(channel < per_slot - 1)
    def _():
        for slot, block in blocks:
            free = lanes_of((capacity, width)) >= kept
            moved = pltpu.roll(cut[slot], kept - channel * piece, 1)
            tri_ref[slot, place, :] = jnp.where(free, moved, block[:capacity]).astype(BF16)


def triangle(contract, rows_n, cols_n, unit, q, p, pairs, name):
    slots, units, capacity, width = pairs.shape
    per_slot = units // p * q // 2
    shape = (slots, returned_rows(capacity, per_slot, q), width)
    cut = (slots, capacity, width) if q > 1 else (1, 8, width)
    return pl.pallas_call(
        functools.partial(triangle_kernel, contract, rows_n, cols_n, unit, q, p),
        grid=(per_slot,),
        in_specs=[pl.BlockSpec(pairs.shape, lambda c: (0, 0, 0, 0))],
        out_specs=pl.BlockSpec(shape, lambda c: (0, 0, 0)),
        out_shape=jax.ShapeDtypeStruct(shape, BF16),
        scratch_shapes=[pltpu.VMEM((2, rows_n * unit, cols_n * width), BF16), pltpu.VMEM(cut, F32)],
        name=name,
    )(pairs)


SMEM = pl.BlockSpec(memory_space=pltpu.SMEM)
ANY = pl.BlockSpec(memory_space=pl.ANY)


def whole_block(array):
    zeros = (0,) * array.ndim
    return pl.BlockSpec(array.shape, lambda g: zeros)


def update_block(array, number):
    index = (number,) + (0,) * (array.ndim - 1)
    return pl.BlockSpec((1,) + array.shape[1:], lambda g: index)


def rows_block(*rest):
    zeros = (0,) * len(rest)
    return pl.BlockSpec((GROUP,) + rest, lambda g: (g,) + zeros)


def with_capacity(
    capacity,
    counts,
    template_pair,
    trunk,
    coverage,
    chain_ids,
    chain_vec,
    trunk_weights,
    proj_weights,
    out_weights,
    final_weights,
):
    unit, trunk_channels, tile_cols = trunk.shape
    channels = template_pair.shape[2]
    rows_n, cols_n = lax.axis_size("row"), lax.axis_size("col")
    slots = rows_n * cols_n
    per_slot = channels // slots
    grid = (pl.cdiv(capacity, GROUP),)
    q, p = packing(capacity, unit, tile_cols, per_slot)
    chain_all = chain_ids[None]
    chain_row = chain_vec[None]

    units = 2 * per_slot // q * p
    pair_spec = pl.BlockSpec((slots, units, GROUP, tile_cols), lambda g: (0, 0, g, 0))
    pair_shape = jax.ShapeDtypeStruct((slots, units, capacity, tile_cols), BF16)
    rep_spec = rows_block(channels, tile_cols)
    rep_shape = jax.ShapeDtypeStruct((capacity, channels, tile_cols), BF16)
    finish_rows = 2 * GROUP if unit % (2 * GROUP) == 0 else GROUP
    finish_spec = pl.BlockSpec((finish_rows, trunk_channels, tile_cols), lambda g: (g, 0, 0))
    tri_spec = pl.BlockSpec((slots, returned_rows(capacity, per_slot, q), tile_cols), lambda g: (0, 0, 0))
    scratch = pltpu.VMEM((2, GROUP * (channels + PAD), tile_cols), F32)
    tri_scratch = pltpu.VMEM((channels * (GROUP + PAD), tile_cols), F32)
    gated_outs = dict(
        out_specs=[pair_spec, rep_spec, rep_spec], out_shape=[pair_shape, rep_shape, rep_shape]
    )

    def exchange(values):
        return lax.all_to_all(values, ("row", "col"), 0, 0, tiled=True)

    pairs, rep, gate = pl.pallas_call(
        functools.partial(pre_kernel, unit, q, p),
        grid=grid,
        in_specs=[
            SMEM,
            SMEM,
            SMEM,
            ANY,
            ANY,
            whole_block(coverage),
            whole_block(chain_all),
            whole_block(chain_row),
            whole_block(trunk_weights),
            update_block(proj_weights, 0),
        ],
        scratch_shapes=[
            scratch,
            pltpu.VMEM((2, GROUP, channels, tile_cols), BF16),
            pltpu.VMEM((2, GROUP, trunk_channels, tile_cols), BF16),
            pltpu.SMEM((unit,), jnp.int32),
            pltpu.VMEM((tile_cols, tile_cols), BF16),
            pltpu.SemaphoreType.DMA((2, 2, GROUP)),
        ],
        name="pre",
        **gated_outs,
    )(coverage, chain_ids, counts, template_pair, trunk, coverage, chain_all, chain_row, trunk_weights, proj_weights)

    tri = exchange(triangle(1, rows_n, cols_n, unit, q, p, exchange(pairs), "outgoing"))
    pairs, rep, gate = pl.pallas_call(
        functools.partial(mid_kernel, unit, capacity, q, p),
        grid=grid,
        in_specs=[SMEM, tri_spec, rep_spec, rep_spec, update_block(out_weights, 0), update_block(proj_weights, 1)],
        scratch_shapes=[scratch, tri_scratch],
        name="mid",
        **gated_outs,
    )(counts, tri, rep, gate, out_weights, proj_weights)

    tri = exchange(triangle(0, rows_n, cols_n, unit, q, p, exchange(pairs), "incoming"))
    pooled = pl.pallas_call(
        functools.partial(last_kernel, capacity, q),
        grid=grid,
        in_specs=[tri_spec, rep_spec, rep_spec, update_block(out_weights, 1)],
        out_specs=rep_spec,
        out_shape=rep_shape,
        scratch_shapes=[tri_scratch],
        name="last",
    )(tri, rep, gate, out_weights)

    other = lax.ppermute(pooled, "tmpl", [(0, 1), (1, 0)])
    return pl.pallas_call(
        functools.partial(finish_kernel, unit),
        grid=(unit // finish_rows,),
        in_specs=[
            SMEM,
            whole_block(pooled),
            whole_block(pooled),
            finish_spec,
            whole_block(coverage),
            whole_block(final_weights),
        ],
        out_specs=finish_spec,
        out_shape=jax.ShapeDtypeStruct(trunk.shape, BF16),
        scratch_shapes=[pltpu.SMEM((2, unit), jnp.int32), pltpu.VMEM((2 * tile_cols, tile_cols), BF16)],
        name="finish",
    )(coverage, pooled, other, trunk, coverage, final_weights)


def per_device(template_pair, trunk, coverage, *rest):
    unit, _, tile_cols = trunk.shape
    templates, tokens = coverage.shape
    counts = jnp.sum(coverage.reshape(templates, tokens // unit, unit), axis=2)
    capacities = [unit]
    if unit == tile_cols and unit % 16 == 0:
        capacities = [unit * share // 16 for share in (12, 13, 14, 16)]
    args = (counts, template_pair, trunk, coverage) + rest
    if len(capacities) == 1:
        return with_capacity(unit, *args)
    most = jnp.max(counts)
    branch = sum((most > capacity).astype(jnp.int32) for capacity in capacities[:-1])
    return lax.switch(branch, [functools.partial(with_capacity, capacity) for capacity in capacities], *args)


def solution(mesh):
    in_specs = (
        P("tmpl", "row", None, "col"),
        P("row", None, "col"),
        P(),
        P(),
        P(),
        P(),
        P(),
        P(),
        P(),
    )
    out_specs = P("row", None, "col")
    return jax.shard_map(
        per_device, mesh=mesh, in_specs=in_specs, out_specs=out_specs, check_vma=False
    )
```
